128 devices in a mesh: seq: 64 (over x, z, y_hi, core), chan: 2 (over y_lo).
Axes of the slice: x: 4, y: 4 (y_hi: 2, y_lo: 2; y = y_hi * 2 + y_lo), z: 4, core: 2. Of those that a mesh axis runs over, the one named last changes fastest.
Arguments:
- signal: bfloat16 [524288, 256], P('seq', 'chan'), parts along dimension 1, may hold values from -6 to 6
- gate_values: bfloat16 [524288, 256], P('seq', 'chan'), parts along dimension 1, may hold values from -4 to 4
- skip_gain: float32 [256], P('chan'), parts along dimension 0, may hold values from 0.25 to 2
- filter_spectrum: bfloat16 [2, 512, 1024, 256], P(None, 'seq', None, 'chan'), parts along dimension 3, may hold values from -4 to 4, as said below
Outputs:
- gated_output: bfloat16 [524288, 256], P('seq', 'chan'), parts along dimension 1
The draws below stay inside these ranges and needn't reach their ends.
There are 2 independent parts, one for each index of `chan`. The reference program is written for one: setup_inputs(seed, part) draws one part's arguments, and reference() takes and returns one part's arrays. A program takes and returns all parts, laid end to end along the dimension named above; each array names one. Nothing has to cross between parts.
Inputs may be any that keep to these rules, and one draw needn't show every extreme that they name: `filter_spectrum`: the spectrum of a real filter: the complex entry at frequency k equals the conjugate of the entry at frequency (524288 - k) mod 524288.
All inputs are finite; a program needn't handle non-finite values.
Results may differ from the reference program's by a relative error of at most 0.0085.
Values may be sent and summed in bfloat16 or wider, within the bound.
A program may use at most 128 MiB of HBM per device.

```python
import math
import jax
import jax.numpy as jnp
from jax import lax

OUTER = 1024
INNER = 512
CH = 128
SEQ = 524288


def draw_filter_spectrum(key, part):
    length = INNER * OUTER
    first_key = jax.random.fold_in(key, 11)
    base = jax.random.normal(first_key, (2, length, CH), jnp.float32)
    mirror = jnp.roll(jnp.flip(base, axis=1), 1, axis=1)
    real_part = (base[0] + mirror[0]) * 0.7071
    imag_part = (base[1] - mirror[1]) * 0.7071
    both = jnp.clip(jnp.stack([real_part, imag_part]), -4.0, 4.0)
    return both.reshape(2, INNER, OUTER, CH).astype(jnp.bfloat16)


def level_of(rng, extent, split, smallest, top_value):
    factor_of = 1.0
    for axis_at, blocks in split:
        heights = jax.random.uniform(jax.random.fold_in(jax.random.fold_in(rng, 6), axis_at), (blocks,), jnp.float32, smallest / len(split), top_value / len(split))
        factor_of = factor_of * jnp.repeat(jnp.exp(heights), extent[axis_at] // blocks).reshape((-1,) + (1,) * (len(extent) - 1 - axis_at))
    return factor_of


def centred(rng, extent, scale, limit, cuts=(), held_as=jnp.bfloat16):
    level = level_of(rng, extent, cuts, -0.22, 0.18) if cuts else 1.0
    values = jax.random.normal(rng, extent, jnp.float32) * scale * level
    return jnp.minimum(jnp.maximum(values, -limit), limit).astype(held_as)


def setup_inputs(seed: int = 0, part: int = 0) -> dict:
    keys = jax.random.split(jax.random.key(seed), 5)
    part_keys = jax.random.split(jax.random.fold_in(keys[4], part), 5)
    signal = centred(part_keys[0], (SEQ, CH), 1.0, 6.0, ((0, 64),))
    gate_values = centred(part_keys[1], (SEQ, CH), 1.0, 4.0, ((0, 64),))
    skip_gain = jnp.clip(jnp.exp(jax.random.uniform(part_keys[2], (CH,), jnp.float32, math.log(0.25), math.log(2.0))), 0.25, 2.0)
    filter_spectrum = draw_filter_spectrum(jax.random.fold_in(jax.random.fold_in(keys[4], part), 71), part)
    return {"signal": signal, "gate_values": gate_values, "skip_gain": skip_gain, "filter_spectrum": filter_spectrum}


def tables(length):
    indices = lax.iota(jnp.int32, length)
    angles = 2.0 * math.pi / length * (indices[:, None] * indices[None, :] % length).astype(jnp.float32)
    return (jnp.cos(angles).astype(jnp.bfloat16), jnp.sin(angles).astype(jnp.bfloat16))

def twiddle(c_values, b_values, length):
    angles = 2.0 * math.pi / length * (c_values[:, None] * b_values[None, :] % length).astype(jnp.float32)
    return (jnp.cos(angles), jnp.sin(angles))

def convolve(operands):
    pieces, filter_cols = operands
    cos_a, sin_a = tables(OUTER)
    cos_b, sin_b = tables(INNER)
    inner_table = jnp.stack([cos_b, sin_b]).astype(jnp.float32)
    tw_cos, tw_sin = twiddle(lax.iota(jnp.int32, OUTER), lax.iota(jnp.int32, INNER), SEQ)
    tw_cos = tw_cos[:, :, None]
    tw_sin = tw_sin[:, :, None]
    outer_scale = 1.0 / math.sqrt(OUTER)
    inner_scale = 1.0 / math.sqrt(INNER)
    breadth = pieces.shape[2]
    flattened = pieces.reshape(OUTER, INNER * breadth)
    fwd_re = jnp.dot(cos_a, flattened, preferred_element_type=jnp.float32).reshape(OUTER, INNER, breadth)
    fwd_im = -jnp.dot(sin_a, flattened, preferred_element_type=jnp.float32).reshape(OUTER, INNER, breadth)
    twisted = jnp.stack([(fwd_re * tw_cos + fwd_im * tw_sin) * outer_scale, (fwd_im * tw_cos - fwd_re * tw_sin) * outer_scale]).astype(jnp.bfloat16)
    partials = jnp.einsum('tdb,scbk->tscdk', inner_table, twisted.astype(jnp.float32), precision=lax.Precision.HIGHEST)
    spectrum = jnp.stack([(partials[0, 0] + partials[1, 1]) * inner_scale, (partials[0, 1] - partials[1, 0]) * inner_scale]).astype(jnp.bfloat16)
    filter_re = jnp.swapaxes(filter_cols[0], 0, 1).astype(jnp.float32)
    filter_im = jnp.swapaxes(filter_cols[1], 0, 1).astype(jnp.float32)
    spec_re = spectrum[0].astype(jnp.float32)
    spec_im = spectrum[1].astype(jnp.float32)
    product = jnp.stack([spec_re * filter_re - spec_im * filter_im, spec_re * filter_im + spec_im * filter_re]).astype(jnp.bfloat16)
    partials = jnp.einsum('tbd,scdk->tscbk', inner_table, product.astype(jnp.float32), precision=lax.Precision.HIGHEST)
    back_re = (partials[0, 0] - partials[1, 1]) * inner_scale
    back_im = (partials[0, 1] + partials[1, 0]) * inner_scale
    rotated_re = (back_re * tw_cos - back_im * tw_sin).astype(jnp.bfloat16)
    rotated_im = (back_re * tw_sin + back_im * tw_cos).astype(jnp.bfloat16)
    convolved = (jnp.dot(cos_a, rotated_re.reshape(OUTER, INNER * breadth), preferred_element_type=jnp.float32) - jnp.dot(sin_a, rotated_im.reshape(OUTER, INNER * breadth), preferred_element_type=jnp.float32)) * outer_scale
    return convolved.reshape(OUTER, INNER, breadth).astype(jnp.bfloat16)

def reference(signal, gate_values, skip_gain, filter_spectrum):
    channels = signal.shape[1]
    group_width = 16 if channels % 16 == 0 else channels
    groups = channels // group_width
    signal_grid = signal.reshape(OUTER, INNER, groups, group_width).transpose(2, 0, 1, 3)
    filter_grid = filter_spectrum.reshape(2, INNER, OUTER, groups, group_width).transpose(3, 0, 1, 2, 4)
    convolved = lax.map(convolve, (signal_grid, filter_grid))
    convolved = convolved.transpose(1, 2, 0, 3).reshape(SEQ, channels)
    result = gate_values.astype(jnp.float32) * (convolved.astype(jnp.float32) + skip_gain[None, :].astype(jnp.float32) * signal.astype(jnp.float32))
    return result.astype(jnp.bfloat16)
```

```python
import math

import jax
import jax.numpy as jnp
import numpy as np
from jax import lax
from jax.experimental import pallas as pl
from jax.experimental.pallas import tpu as pltpu
from jax.sharding import PartitionSpec as P

MESH = pl.DeviceIdType.MESH
N = 64
H = N - 1
MULT = 27
OUTER = 1024
INNER = 512
SEQ = OUTER * INNER
BF = jnp.bfloat16
F32 = jnp.float32
SCALE = 1.0 / SEQ


def _circle(index, length):
    angle = 2.0 * np.pi / length * (index % length)
    return np.cos(angle), np.sin(angle)


def make_tables():
    a = np.arange(OUTER)
    c = np.arange(INNER)
    cos, sin = _circle(np.outer(c, a), OUTER)
    alt = 1.0 - 2.0 * (a % 2)
    fwd = np.stack([cos, -sin], 1)
    fwd[0, 1] = alt
    t1 = fwd.reshape(N, 8, 2, OUTER).transpose(0, 2, 1, 3).reshape(N, 16, OUTER)
    inv = 2.0 * fwd
    inv[0] = fwd[0]
    t4 = inv.reshape(N, 2, 4, 2, OUTER).transpose(1, 0, 2, 3, 4).reshape(1024, OUTER).T
    t4 = t4.reshape(N, 16, 1024)
    d = np.arange(INNER)
    cos, sin = _circle(np.outer(d, d), INNER)
    t2 = np.stack([np.stack([cos, sin], 0), np.stack([-sin, cos], 0)], 0)

    def blocks(m):
        m = m.reshape(2, 2, N, 8, N, 8).transpose(2, 0, 3, 4, 1, 5)
        return m.reshape(N, 16, 1024)

    d = np.arange(256)
    b = np.arange(INNER)
    cos0, sin0 = _circle(np.outer(d, b), INNER)
    cosh, sinh = _circle(np.outer(2 * d + 1, b), 2 * INNER)
    altb = 1.0 - 2.0 * (b % 2)
    s2 = np.zeros((2, 2, INNER, INNER))
    s2[0, 0, :256] = cos0
    s2[1, 0, :256] = -sin0
    s2[1, 0, 0] = altb
    s2[0, 1, 256:] = cosh
    s2[1, 1, 256:] = -sinh
    s3 = np.zeros((2, 2, INNER, INNER))
    s3[0, 0, :, :256] = 2 * cos0.T
    s3[0, 1, :, :256] = 2 * sin0.T
    s3[0, 0, :, 0] = 1.0
    s3[0, 1, :, 0] = -altb
    s3[1, 0, :, 256:] = -2 * cosh.T
    s3[1, 1, :, 256:] = -2 * sinh.T
    return t1, blocks(t2), blocks(s2), blocks(s3), t4


def peer(me, k):
    k = lax.rem(k * MULT, N)
    return (
        lax.rem(me // 16 + k // 16, 4) * 16
        + lax.rem(me // 4 + k // 4, 4) * 4
        + lax.rem(me // 2 + k // 2, 2) * 2
        + lax.rem(me + k, 2)
    )


def source(me, k):
    k = lax.rem(k * MULT, N)
    return (
        lax.rem(me // 16 + 4 - k // 16, 4) * 16
        + lax.rem(me // 4 + 16 - k // 4, 4) * 4
        + lax.rem(me // 2 + N - k // 2, 2) * 2
        + lax.rem(me + N - k, 2)
    )


def dot(x, y):
    return jnp.dot(x, y, preferred_element_type=F32)


def loop(n, body, start=0):
    def step(i, carry):
        body(i)
        return carry

    lax.fori_loop(start, n, step, 0)


def kernel(
    sig_h, filt_h, gate_h, skip, wt, t1_h, t2_h, t2s_h, t3s_h, t4_h, out_h,
    x1, fr, xf, x2, x4, x5, y2, y3, y4,
    t1, t2, t2s, t3s, t4, wb, fw, nyq, xb, tr, acc, prod, part, sig, gate, outv,
    ss, rs, ls,
):
    me = lax.axis_index("seq")
    ch = lax.axis_index("chan")
    bar = pltpu.get_barrier_semaphore()

    def hello(k):
        pl.semaphore_signal(bar, inc=1, device_id=(peer(me, k), ch), device_id_type=MESH)

    loop(N, hello, 1)
    pl.semaphore_wait(bar, H)

    def remote(src, dst, s, r, p):
        return pltpu.make_async_remote_copy(
            src, dst, ss.at[s], rs.at[r], device_id=(p, ch), device_id_type=MESH
        )

    def wait_recv(r, ref):
        remote(ref, ref, 0, r, me).wait_recv()

    def wait_send(s, ref):
        remote(ref, ref, s, 0, me).wait_send()

    def copy(src, dst, s):
        return pltpu.make_async_copy(src, dst, ls.at[s])

    def send1(k):
        p = peer(me, k)
        remote(sig_h.at[:, p], x1.at[me], 0, 0, p).start()

    loop(N, send1, 1)
    own1 = copy(sig_h.at[:, me], x1.at[me], 0)
    own1.start()

    def send_f(k):
        p = peer(me, k)
        remote(filt_h.at[:, :, p], fr.at[me], 1, 1, p).start()

    loop(N, send_f, 1)
    own_f = copy(filt_h.at[:, :, me], fr.at[me], 1)
    own_f.start()

    @pl.when(me == 0)
    def _():
        copy(filt_h.at[:, :, N], xf.at[0], 8).start()

    @pl.when((me > 0) & (me < 32))
    def _():
        remote(filt_h.at[:, :, N], xf.at[me], 2, 2, 0).start()

    special = 1 - jnp.minimum(me, 1)

    def load_tables(k):
        p = peer(me, k)
        copy(t1_h.at[p], t1.at[k], 2).start()
        copy(t2_h.at[p], t2.at[k], 3).start()
        copy(t2s_h.at[special, p], t2s.at[k], 4).start()
        copy(t3s_h.at[special, p], t3s.at[k], 5).start()
        copy(t4_h.at[p], t4.at[k], 6).start()

    loop(N, load_tables)
    sig_in = copy(sig_h, sig, 7)
    gate_in = copy(gate_h, gate, 9)
    sig_in.start()
    gate_in.start()

    def spread(u):
        w = wt[u]
        for j in range(16):
            wb[u, j] = jnp.broadcast_to(w[:, j : j + 1], (8, 128))

    loop(N, spread)

    def table_wait(ref, s):
        copy(ref, ref, s).wait()

    table_wait(t1, 2)
    table_wait(t2, 3)
    table_wait(t2s, 4)
    table_wait(t3s, 5)
    table_wait(t4, 6)

    wait_recv(0, x1.at[pl.ds(0, H)])
    own1.wait()

    def relay1(i):
        v = x1[pl.ds(i * 8, 8)].astype(F32).reshape(1024, 128)
        tr[...] = v
        for b in range(8):
            xb[pl.ds(pl.multiple_of(i * 128, 128), 128), b * 128 : (b + 1) * 128] = tr[
                pl.ds(b, 128, stride=8), :
            ].astype(BF)

    loop(8, relay1)

    def stage1(g):
        acc[...] = dot(t1[pl.ds(g * 16, 16)].reshape(256, 1024), xb[...])

        def twist(i):
            k = g * 16 + i
            u = peer(me, k)
            r0 = pl.multiple_of(i * 16, 16)
            base = 0
            for b in range(8):
                re = acc[pl.ds(r0, 8), b * 128 : (b + 1) * 128]
                im = acc[pl.ds(r0 + 8, 8), b * 128 : (b + 1) * 128]
                wc = wb[u, b]
                ws = wb[u, 8 + b]
                tr[pl.ds(base + b, 8, stride=16), :] = re * wc + im * ws
                tr[pl.ds(base + 8 + b, 8, stride=16), :] = im * wc - re * ws
            y2[k] = tr[0:128, :].reshape(8, 16, 128).astype(BF)

        loop(16, twist)

        def send2(i):
            k = g * 16 + i
            p = peer(me, k)

            @pl.when(k > 0)
            def _():
                remote(y2.at[k, pl.ds(0, 4)], x2.at[pl.ds(0, 4), me], 3, 3, p).start()

        loop(16, send2)

    loop(4, stage1)

    def send2b(k):
        p = peer(me, k)
        remote(y2.at[k, pl.ds(4, 4)], x2.at[pl.ds(4, 4), me], 4, 4, p).start()

    loop(N, send2b, 1)
    for j in range(8):
        x2[j, me] = y2[0, j]

    wait_recv(1, fr.at[pl.ds(0, H)])
    own_f.wait()

    def relay_f(v):
        tr[0:128, :] = fr[v].astype(F32).reshape(128, 128)
        for c in range(8):
            fw[c, v] = tr[pl.ds(c, 16, stride=8), :].astype(BF)

    loop(N, relay_f)

    @pl.when(me == 0)
    def _():
        copy(filt_h.at[:, :, N], xf.at[0], 8).wait()
        wait_recv(2, xf.at[pl.ds(0, 31)])
        nyq[...] = fw[0, 32].astype(F32)

        def relay_x(v):
            tr[0:128, :] = xf[v].astype(F32).reshape(128, 128)
            fw[0, 32 + v] = tr[pl.ds(0, 16, stride=8), :].astype(BF)

        loop(32, relay_x)

    for h in range(2):
        wait_recv(3 + h, x2.at[pl.ds(4 * h, 4), pl.ds(0, H)])
        cols = [x2[4 * h + j].reshape(1024, 128) for j in range(4)]
        for j in range(4):
            xb[:, j * 128 : (j + 1) * 128] = cols[j]

        def stage2(g):
            tab = t2[pl.ds(g * 16, 16)].reshape(256, 1024)
            if h == 0:
                tabs = t2s[pl.ds(g * 16, 16)].reshape(256, 1024)
                acc[:, 0:128] = dot(tabs, xb[:, 0:128])
                acc[:, 128:512] = dot(tab, xb[:, 128:512])
            else:
                acc[:, 0:512] = dot(tab, xb[:, 0:512])

            def multiply(i):
                v = peer(me, g * 16 + i)
                r0 = pl.multiple_of(i * 16, 16)
                for j in range(4):
                    sr = acc[pl.ds(r0, 8), j * 128 : (j + 1) * 128]
                    si = acc[pl.ds(r0 + 8, 8), j * 128 : (j + 1) * 128]
                    f = fw[4 * h + j, v].astype(F32)
                    fre = f[0:8]
                    fim = f[8:16]
                    pr = sr * fre - si * fim
                    pi = -(sr * fim + si * fre)
                    prod[pl.ds(pl.multiple_of(v * 16, 16), 16), j * 128 : (j + 1) * 128] = (
                        jnp.concatenate([pr, pi], axis=0).astype(BF)
                    )

            loop(16, multiply)
            if h == 0:

                @pl.when((me == 0) & (g == 0))
                def _():
                    sr = acc[0:8, 0:128]
                    si = acc[8:16, 0:128]
                    f = fw[0, 0].astype(F32)
                    fre = f[0:8]
                    fim = f[8:16]
                    rows = lax.broadcasted_iota(jnp.int32, (8, 128), 0)
                    pr = sr * fre - si * fim
                    pi = -(sr * fim + si * fre)
                    pr = jnp.where(rows == 0, sr * fre, pr)
                    pi = jnp.where(rows == 0, -(si * nyq[0:8]), pi)
                    prod[0:16, 0:128] = jnp.concatenate([pr, pi], axis=0).astype(BF)

        loop(4, stage2)

        def stage3(g):
            tab = t2[pl.ds(g * 16, 16)].reshape(256, 1024)
            if h == 0:
                tabs = t3s[pl.ds(g * 16, 16)].reshape(256, 1024)
                acc[:, 0:128] = dot(tabs, prod[:, 0:128])
                acc[:, 128:512] = dot(tab, prod[:, 128:512])
            else:
                acc[:, 0:512] = dot(tab, prod[...])

            def untwist(i):
                k = g * 16 + i
                t = peer(me, k)
                r0 = pl.multiple_of(i * 16, 16)
                for j in range(4):
                    re = acc[pl.ds(r0, 8), j * 128 : (j + 1) * 128]
                    im = acc[pl.ds(r0 + 8, 8), j * 128 : (j + 1) * 128]
                    wc = wb[t, 4 * h + j]
                    ws = wb[t, 8 + 4 * h + j]
                    y3[k, 4 * h + j] = jnp.concatenate(
                        [re * wc + im * ws, re * ws - im * wc], axis=0
                    ).astype(BF)

            loop(16, untwist)

            def send3(i):
                k = g * 16 + i
                p = peer(me, k)

                @pl.when(k > 0)
                def _():
                    remote(
                        y3.at[k, pl.ds(4 * h, 4)], x4.at[me, pl.ds(4 * h, 4)], 5 + h, 5 + h, p
                    ).start()

            loop(16, send3)

        loop(4, stage3)
        for j in range(4):
            x4[me, 4 * h + j] = y3[0, 4 * h + j]

    for h in range(2):
        wait_recv(5 + h, x4.at[pl.ds(0, H), pl.ds(4 * h, 4)])

        def relay4(i):
            v = x4[pl.ds(i * 2, 2), 4 * h : 4 * h + 4].astype(F32).reshape(128, 128)
            tr[0:128, :] = v
            for b in range(8):
                xb[pl.ds(pl.multiple_of(h * 512 + i * 16, 16), 16), b * 128 : (b + 1) * 128] = tr[
                    pl.ds(b, 16, stride=8), :
                ].astype(BF)

        loop(32, relay4)

        def stage4(g):
            rows = pl.ds(pl.multiple_of(g * 256, 256), 256)
            if h == 0:
                part[rows, :] = dot(
                    t4[pl.ds(g * 16, 16), :, 0:512].reshape(256, 512), xb[0:512, :]
                )
                return
            acc[...] = part[rows, :] + dot(
                t4[pl.ds(g * 16, 16), :, 512:1024].reshape(256, 512), xb[512:1024, :]
            )

            def finish(i):
                k = g * 16 + i
                r0 = pl.multiple_of(i * 16, 16)
                for b in range(8):
                    tr[pl.ds(b, 16, stride=8), :] = acc[pl.ds(r0, 16), b * 128 : (b + 1) * 128]
                y4[k] = (tr[0:128, :] * SCALE).reshape(16, 8, 128).astype(BF)

            loop(16, finish)

            def send4(i):
                k = g * 16 + i
                p = peer(me, k)

                @pl.when(k > 0)
                def _():
                    remote(y4.at[k], x5.at[me], 7, 7 + g, p).start()

            loop(16, send4)

        loop(4, stage4)

    x5[me] = y4[0]
    sig_in.wait()
    gate_in.wait()
    gain = skip[0:1, :].reshape(1, 1, 128)

    def last(g):
        if isinstance(g, int) and g == 0:
            wait_recv(7, x5.at[pl.ds(0, 15)])
        else:
            wait_recv(7 + g, x5.at[pl.ds(0, 16)])

        def gated(i):
            t = source(me, g * 16 + i)
            y = x5[t].astype(F32) + gain * sig[:, t].astype(F32)
            outv[:, t] = (gate[:, t].astype(F32) * y).astype(BF)

        loop(16, gated)

    for g in range(4):
        last(g)
    done = copy(outv, out_h, 10)
    done.start()
    wait_send(0, sig_h.at[:, pl.ds(0, H)])
    wait_send(1, filt_h.at[:, :, pl.ds(0, H)])

    @pl.when((me > 0) & (me < 32))
    def _():
        wait_send(2, filt_h.at[:, :, N])

    for h in range(2):
        wait_send(3 + h, y2.at[pl.ds(0, H), pl.ds(4 * h, 4)])
        wait_send(5 + h, y3.at[pl.ds(0, H), pl.ds(4 * h, 4)])
    wait_send(7, y4.at[pl.ds(0, H)])
    done.wait()


def local(signal, gate_values, skip_gain, filter_spectrum):
    me = lax.axis_index("seq")
    rows = lax.iota(jnp.int32, INNER)[:, None]
    lane = lax.iota(jnp.int32, 128)[None, :]
    own = me * 8 + lane % 8
    angle = 2.0 * math.pi / SEQ * (rows * own).astype(F32)
    wt = jnp.where(lane < 8, jnp.cos(angle), jnp.sin(angle)).reshape(N, 8, 128)
    t1, t2, s2, s3, t4 = make_tables()
    t2s = jnp.asarray(np.stack([t2, s2]), BF)
    t3s = jnp.asarray(np.stack([t2, s3]), BF)
    tabs = [jnp.asarray(t1, BF), jnp.asarray(t2, BF), t2s, t3s, jnp.asarray(t4, BF)]
    any_ = pl.BlockSpec(memory_space=pl.ANY)
    vm = pl.BlockSpec(memory_space=pltpu.VMEM)
    V = pltpu.VMEM
    dma = pltpu.SemaphoreType.DMA
    out = pl.pallas_call(
        kernel,
        out_shape=jax.ShapeDtypeStruct((16, 64, 8, 128), BF),
        in_specs=[any_, any_, any_, vm, vm] + [any_] * 5,
        out_specs=any_,
        scratch_shapes=[
            V((64, 16, 8, 128), BF),
            V((64, 2, 8, 8, 128), BF),
            V((32, 2, 8, 8, 128), BF),
            V((8, 64, 16, 128), BF),
            V((64, 8, 16, 128), BF),
            V((64, 16, 8, 128), BF),
            V((64, 8, 16, 128), BF),
            V((64, 8, 16, 128), BF),
            V((64, 16, 8, 128), BF),
            V((64, 16, 1024), BF),
            V((64, 16, 1024), BF),
            V((64, 16, 1024), BF),
            V((64, 16, 1024), BF),
            V((64, 16, 1024), BF),
            V((64, 16, 8, 128), F32),
            V((8, 64, 16, 128), BF),
            V((16, 128), F32),
            V((1024, 1024), BF),
            V((1024, 128), F32),
            V((256, 1024), F32),
            V((1024, 512), BF),
            V((1024, 1024), F32),
            V((16, 64, 8, 128), BF),
            V((16, 64, 8, 128), BF),
            V((16, 64, 8, 128), BF),
            dma((8,)),
            dma((12,)),
            dma((12,)),
        ],
        compiler_params=pltpu.CompilerParams(
            collective_id=0, has_side_effects=True, vmem_limit_bytes=67043328
        ),
    )(
        signal.reshape(16, 64, 8, 128),
        filter_spectrum.reshape(2, 8, 128, 8, 128),
        gate_values.reshape(16, 64, 8, 128),
        skip_gain.reshape(1, 128),
        wt,
        *tabs,
    )
    return out.reshape(8192, 128)


def solution(mesh):
    return jax.shard_map(
        local,
        mesh=mesh,
        in_specs=(P("seq", "chan"), P("seq", "chan"), P("chan"), P(None, "seq", None, "chan")),
        out_specs=P("seq", "chan"),
        check_vma=False,
    )
```

```python
import math

import jax
import jax.numpy as jnp
import numpy as np
from jax import lax
from jax.experimental import pallas as pl
from jax.experimental.pallas import tpu as pltpu
from jax.sharding import PartitionSpec as P

MESH = pl.DeviceIdType.MESH
N = 64
H = N - 1
MULT = 27
OUTER = 1024
INNER = 512
SEQ = OUTER * INNER
BF = jnp.bfloat16
F32 = jnp.float32
SCALE = 1.0 / SEQ


def _circle(index, length):
    angle = 2.0 * np.pi / length * (index % length)
    return np.cos(angle), np.sin(angle)


def make_tables():
    pi = np.pi
    rows = np.arange(N)[:, None]
    lane = np.arange(128)[None, :]
    q = np.arange(16)[:, None]
    ro, x8 = q // 8, q % 8
    col = np.arange(1024)[None, :]
    a1 = 2 * pi / 128 * (rows * lane % 128)
    b1 = 2 * pi / 1024 * (x8 * col % 1024) + ro * pi / 2
    x = lane // 16 * 8 + lane % 8
    a2 = 2 * pi / 64 * (rows * x % 64)
    y = col // 16 * 8 + col % 8
    ri = col // 8 % 2
    b2 = 2 * pi / 512 * (x8 * y % 512) + (ro - ri) * pi / 2
    hh, u, c4, r4 = col // 512, col // 8 % 64, col // 2 % 4, col % 2
    c = 8 * u + 4 * hh + c4
    a4 = [2 * pi / 64 * (rows * c[:, h * 512 : h * 512 + 128] % 64) for h in range(2)]
    b4 = 2 * pi / 1024 * (q * c % 1024) + r4 * pi / 2
    half = 2 * pi / 1024 * y
    lo = (ri == 0) * np.ones((16, 1))
    hi = (ri == 1) * np.ones((16, 1))
    b2hi = b2 + ri * (pi / 2 + half)
    a3 = a2 + pi / 64 * rows
    up = col >= 512
    b3 = b2 + up * (pi / 1024 * 2 * x8 + pi)
    b3 = b3 - up * ro * pi / 2 + 0.0
    w3 = 2.0 * np.where(up, ro == 1, ro == 0)
    f = lambda m, w=1.0: np.stack([np.cos(m) * w, np.sin(m) * w])
    blocks = np.stack([f(a1), f(a2), f(a3), f(a4[0]), f(a4[1])])
    inner = np.stack(
        [f(b1), f(b2), f(b2, lo), f(b2hi, hi), f(b3, w3), f(b4, 2.0)]
    )
    return blocks.astype(np.float32), inner.astype(np.float32)


def peer(me, k):
    k = lax.rem(k * MULT, N)
    return (
        lax.rem(me // 16 + k // 16, 4) * 16
        + lax.rem(me // 4 + k // 4, 4) * 4
        + lax.rem(me // 2 + k // 2, 2) * 2
        + lax.rem(me + k, 2)
    )


def near(me, u):
    def gap(i, j):
        d = lax.rem(j - i + 4, 4)
        return jnp.minimum(d, 4 - d)

    def closer(i, j):
        return jnp.minimum(jnp.maximum(gap(3 - i, j) - gap(i, j), 0), 1)

    x = closer(me // 16, u // 16)
    z = closer(lax.rem(me // 4, 4), lax.rem(u // 4, 4))
    y = 1 - lax.rem(me // 2 + u // 2, 2)
    return x + z + y >= 2


def dot(x, y):
    return jnp.dot(x, y, preferred_element_type=F32)


def loop(n, body, start=0):
    def step(i, carry):
        body(i)
        return carry

    lax.fori_loop(start, n, step, 0)


def kernel(
    sig_h, filt_h, blk_h, inn_h, out_h,
    x1, fv, yd, ym, yq, x2, x4, y2, y3, y4,
    t1, t2, t2s, t3s, t4, wb, fw, nyq, xb, tr, acc, prod, part, blk, inn,
    ss, rs, ls,
):
    me = lax.axis_index("seq")
    ch = lax.axis_index("chan")
    bar = pltpu.get_barrier_semaphore()

    def hello(k):
        pl.semaphore_signal(bar, inc=1, device_id=(peer(me, k), ch), device_id_type=MESH)

    blk_in = pltpu.make_async_copy(blk_h, blk, ls.at[2])
    inn_in = pltpu.make_async_copy(inn_h, inn, ls.at[3])
    blk_in.start()
    inn_in.start()
    fv_in = pltpu.make_async_copy(filt_h, fv, ls.at[1])
    fv_in.start()
    loop(N, hello, 1)
    pl.semaphore_wait(bar, H)

    def remote(src, dst, s, r, p):
        return pltpu.make_async_remote_copy(
            src, dst, ss.at[s], rs.at[r], device_id=(p, ch), device_id_type=MESH
        )

    def wait_recv(r, ref):
        remote(ref, ref, 0, r, me).wait_recv()

    def wait_send(s, ref):
        remote(ref, ref, s, 0, me).wait_send()

    def copy(src, dst, s):
        return pltpu.make_async_copy(src, dst, ls.at[s])

    def send1(k):
        p = peer(me, k)
        remote(sig_h.at[:, p], x1.at[me], 0, 0, p).start()

    loop(N, send1, 1)
    own1 = copy(sig_h.at[:, me], x1.at[me], 0)
    own1.start()

    special = 1 - jnp.minimum(me, 1)
    row = lax.broadcasted_iota(jnp.int32, (16, 128), 0)
    lanes = lax.broadcasted_iota(jnp.int32, (16, 128), 1)

    def factors(i, p):
        return blk[i, 0, pl.ds(p, 1), :], blk[i, 1, pl.ds(p, 1), :]

    def tables(k):
        p = peer(me, k)
        a1 = factors(0, p)
        a2 = factors(1, p)
        a3 = factors(1 + special, p)
        a4 = (factors(3, p), factors(4, p))
        fwd = 1 + special * (1 + p // 32)
        inv = 1 + special * 3
        for j in range(8):
            cols = slice(j * 128, (j + 1) * 128)
            v = a1[0] * inn[0, 0, :, cols] - a1[1] * inn[0, 1, :, cols]
            alt = (1 - 2 * (lanes % 2)).astype(F32)
            v = jnp.where((row == 8) & (p == 0), alt, v)
            t1[k, :, cols] = v.astype(BF)
            v = a2[0] * inn[1, 0, :, cols] - a2[1] * inn[1, 1, :, cols]
            t2[k, :, cols] = v.astype(BF)
            v = a2[0] * inn[fwd, 0, :, cols] - a2[1] * inn[fwd, 1, :, cols]
            real = lanes // 8 % 2 == 0
            v = jnp.where((row == 8) & (p == 0) & (me == 0), jnp.where(real, alt, 0.0), v)
            t2s[k, :, cols] = v.astype(BF)
            a = a2 if j < 4 else a3
            v = a[0] * inn[inv, 0, :, cols] - a[1] * inn[inv, 1, :, cols]
            if j == 0:
                d0 = jnp.where(row < 8, jnp.where(lanes == 0, 1.0, (2 * (row % 2) - 1).astype(F32)), 0.0)
                v = jnp.where(((lanes == 0) | (lanes == 8)) & (me == 0), d0, v)
            t3s[k, :, cols] = v.astype(BF)
            a = a4[j // 4]
            v = a[0] * inn[5, 0, :, cols] - a[1] * inn[5, 1, :, cols]
            if j == 0:
                v = jnp.where(lanes == 0, 1.0, v)
                v = jnp.where(lanes == 1, (1 - 2 * (row % 2)).astype(F32), v)
            t4[k, :, cols] = v.astype(BF)

    blk_in.wait()
    inn_in.wait()
    loop(N, tables)

    def spread(u):
        r8 = lax.broadcasted_iota(jnp.int32, (8, 128), 0)
        l8 = lax.broadcasted_iota(jnp.int32, (8, 128), 1)
        turn = ((u * 8 + r8) * (me * 8 + l8 % 8)).astype(F32) * (2.0 * math.pi / SEQ)
        w = jnp.cos(turn - (l8 // 8).astype(F32) * (math.pi / 2))
        for j in range(16):
            wb[u, j] = jnp.broadcast_to(w[:, j : j + 1], (8, 128))

    loop(N, spread)

    fv_in.wait()
    sign = jnp.where(lax.broadcasted_iota(jnp.int32, (16, 128), 0) < 8, 1.0, -1.0)

    def direct(u):
        tr[0:128, :] = fv[:, :, u].astype(F32).reshape(128, 128)
        for c in range(8):
            yd[u, c] = tr[pl.ds(c, 16, stride=8), :].astype(BF)

    def mirrored(u):
        for p in range(2):
            for d in range(8):
                r = 128 + p * 64 + (7 - d) * 8
                tr[r : r + 8, :] = fv[p, d, 127 - u].astype(F32)
                tr[r + 128 : r + 136, :] = fv[p, d, 128 - u].astype(F32)
        ym[u, 0] = (tr[pl.ds(256, 16, stride=8), :] * sign).astype(BF)
        for c in range(1, 8):
            ym[u, c] = (tr[pl.ds(136 - c, 16, stride=8), :] * sign).astype(BF)

    def send_d(u, h):
        remote(
            yd.at[u, pl.ds(4 * h, 4)], fw.at[pl.ds(4 * h, 4), me], 1 + h, 1 + 10 * h, u
        ).start()

    def send_m(u, h):
        remote(
            ym.at[u, pl.ds(4 * h, 4)], fw.at[pl.ds(4 * h, 4), H - me], 1 + h, 1 + 10 * h, u
        ).start()

    direct(0)

    @pl.when(me >= 32)
    def _():
        tr[0:128, :] = fv[:, :, N].astype(F32).reshape(128, 128)
        yq[...] = yd[0, 0]
        yd[0, 0] = tr[pl.ds(0, 16, stride=8), :].astype(BF)

    @pl.when(me == 32)
    def _():
        remote(yq, nyq, 8, 2, 0).start()

    @pl.when(me > 0)
    def _():
        send_d(0, 0)

    def prepare(k):
        u = peer(me, k)

        @pl.when((u > 0) & near(me, u))
        def _():
            direct(u)
            mirrored(u)

            @pl.when(k > 0)
            def _():
                send_d(u, 0)
                send_m(u, 0)
                send_d(u, 1)
                send_m(u, 1)

    loop(N, prepare)

    def send_later(k):
        u = peer(me, k)

        @pl.when((u > 0) & near(me, u))
        def _():
            send_d(u, 1)
            send_m(u, 1)

    wait_recv(0, x1.at[pl.ds(0, H)])
    own1.wait()

    def relay1(i):
        v = x1[pl.ds(i * 8, 8)].astype(F32).reshape(1024, 128)
        tr[...] = v
        for b in range(8):
            xb[pl.ds(pl.multiple_of(i * 128, 128), 128), b * 128 : (b + 1) * 128] = tr[
                pl.ds(b, 128, stride=8), :
            ].astype(BF)

    loop(8, relay1)

    for j in range(4):
        cols = slice(j * 256, (j + 1) * 256)
        part[:, cols] = dot(t1[...].reshape(1024, 1024), xb[:, cols])

    def stage1(g):

        def send2(i):
            k = g * 16 + i
            p = peer(me, k)

            @pl.when((k > 0) & (i >= 0))
            def _():
                remote(y2.at[k, pl.ds(0, 4)], x2.at[pl.ds(0, 4), me], 3, 3, p).start()

        def twist(i):
            k = g * 16 + i
            u = peer(me, k)
            r0 = pl.multiple_of(k * 16, 16)
            base = 0
            for b in range(8):
                re = part[pl.ds(r0, 8), b * 128 : (b + 1) * 128]
                im = part[pl.ds(r0 + 8, 8), b * 128 : (b + 1) * 128]
                wc = wb[u, b]
                ws = wb[u, 8 + b]
                tr[pl.ds(base + b, 8, stride=16), :] = re * wc + im * ws
                tr[pl.ds(base + 8 + b, 8, stride=16), :] = im * wc - re * ws
            y2[k] = tr[0:128, :].reshape(8, 16, 128).astype(BF)
            send2(i - 1)

        loop(16, twist)
        send2(15)

    loop(4, stage1)

    for j in range(8):
        x2[j, me] = y2[0, j]

    def send2b(k):
        p = peer(me, k)
        remote(y2.at[k, pl.ds(4, 4)], x2.at[pl.ds(4, 4), me], 4, 4, p).start()

    loop(N, send2b, 1)

    @pl.when(me > 0)
    def _():
        send_d(0, 1)

    for c in range(8):
        fw[c, me] = yd[me, c]

    @pl.when(me > 0)
    def _():
        for c in range(8):
            fw[c, H - me] = ym[me, c]

    @pl.when(me == 0)
    def _():
        wait_recv(2, nyq)

    for h in range(2):
        wait_recv(3 + h, x2.at[pl.ds(4 * h, 4), pl.ds(0, H)])

        @pl.when(me == 0)
        def _():
            wait_recv(1 + 10 * h, fw.at[pl.ds(4 * h, 4), pl.ds(0, N - 1)])

        @pl.when(me > 0)
        def _():
            wait_recv(1 + 10 * h, fw.at[pl.ds(4 * h, 4), pl.ds(0, N - 2)])

        cols = [x2[4 * h + j].reshape(1024, 128) for j in range(4)]
        for j in range(4):
            xb[:, j * 128 : (j + 1) * 128] = cols[j]

        def inner(first, ref, at):
            tab = t2[...].reshape(1024, 1024)
            if h == 0:
                part[:, at : at + 128] = dot(first[...].reshape(1024, 1024), ref[:, 0:128])
                part[:, at + 128 : at + 256] = dot(tab, ref[:, 128:256])
            else:
                part[:, at : at + 256] = dot(tab, ref[:, 0:256])
            part[:, at + 256 : at + 512] = dot(tab, ref[:, 256:512])

        inner(t2s, xb, 0)

        def stage2(g):
            def multiply(i):
                v = peer(me, g * 16 + i)
                r0 = pl.multiple_of(g * 256 + i * 16, 16)
                for j in range(4):
                    sr = part[pl.ds(r0, 8), j * 128 : (j + 1) * 128]
                    si = part[pl.ds(r0 + 8, 8), j * 128 : (j + 1) * 128]
                    f = fw[4 * h + j, v].astype(F32)
                    fre = f[0:8]
                    fim = f[8:16]
                    pr = sr * fre - si * fim
                    pi = -(sr * fim + si * fre)
                    prod[pl.ds(pl.multiple_of(v * 16, 16), 16), j * 128 : (j + 1) * 128] = (
                        jnp.concatenate([pr, pi], axis=0).astype(BF)
                    )

            loop(16, multiply)
            if h == 0:

                @pl.when((me == 0) & (g == 0))
                def _():
                    sr = part[0:8, 0:128]
                    si = part[8:16, 0:128]
                    f = fw[0, 0].astype(F32)
                    fre = f[0:8]
                    fim = f[8:16]
                    rows = lax.broadcasted_iota(jnp.int32, (8, 128), 0)
                    pr = sr * fre - si * fim
                    pi = -(sr * fim + si * fre)
                    pr = jnp.where(rows == 0, sr * fre, pr)
                    pi = jnp.where(rows == 0, -(si * nyq[...].astype(F32)[0:8]), pi)
                    prod[0:16, 0:128] = jnp.concatenate([pr, pi], axis=0).astype(BF)

        loop(4, stage2)

        inner(t3s, prod, 512)

        def stage3(g):
            def send3(i):
                k = g * 16 + i
                p = peer(me, k)

                @pl.when((k > 0) & (i >= 0))
                def _():
                    remote(
                        y3.at[k, pl.ds(4 * h, 4)], x4.at[me, pl.ds(4 * h, 4)], 5 + h, 5 + h, p
                    ).start()

            def untwist(i):
                k = g * 16 + i
                t = peer(me, k)
                r0 = pl.multiple_of(k * 16, 16)
                for j in range(4):
                    re = part[pl.ds(r0, 8), 512 + j * 128 : 640 + j * 128]
                    im = part[pl.ds(r0 + 8, 8), 512 + j * 128 : 640 + j * 128]
                    wc = wb[t, 4 * h + j]
                    ws = wb[t, 8 + 4 * h + j]
                    y3[k, 4 * h + j] = jnp.concatenate(
                        [re * wc + im * ws, re * ws - im * wc], axis=0
                    ).astype(BF)
                send3(i - 1)

            loop(16, untwist)
            send3(15)

        loop(4, stage3)
        for j in range(4):
            x4[me, 4 * h + j] = y3[0, 4 * h + j]

    for h in range(2):
        wait_recv(5 + h, x4.at[pl.ds(0, H), pl.ds(4 * h, 4)])

        def relay4(i):
            v = x4[pl.ds(i * 2, 2), 4 * h : 4 * h + 4].astype(F32).reshape(128, 128)
            tr[0:128, :] = v
            for b in range(8):
                xb[pl.ds(pl.multiple_of(h * 512 + i * 16, 16), 16), b * 128 : (b + 1) * 128] = tr[
                    pl.ds(b, 16, stride=8), :
                ].astype(BF)

        loop(32, relay4)

        def stage4(g):
            rows = pl.ds(pl.multiple_of(g * 256, 256), 256)
            acc[...] = part[rows, :] + dot(
                t4[pl.ds(g * 16, 16), :, 512:1024].reshape(256, 512), xb[512:1024, :]
            )

            def send4(i):
                k = g * 16 + i
                p = peer(me, k)

                @pl.when((k > 0) & (i >= 0))
                def _():
                    remote(y4.at[k], out_h.at[:, me], 7, 7, p).start()

            def finish(i):
                k = g * 16 + i
                r0 = pl.multiple_of(i * 16, 16)
                for b in range(8):
                    tr[pl.ds(b, 16, stride=8), :] = acc[pl.ds(r0, 16), b * 128 : (b + 1) * 128]
                y4[k] = (tr[0:128, :] * SCALE).reshape(16, 8, 128).astype(BF)
                send4(i - 1)

            loop(16, finish)
            send4(15)

        if h == 0:
            for j in range(4):
                cols = slice(j * 256, (j + 1) * 256)
                part[:, cols] = dot(t4[:, :, 0:512].reshape(1024, 512), xb[0:512, cols])
        else:
            loop(4, stage4)

    own4 = copy(y4.at[0], out_h.at[:, me], 10)
    own4.start()
    wait_send(0, sig_h.at[:, pl.ds(0, H)])
    near0 = near(me, 0)

    def drained(n):
        for h in range(2):
            wait_send(1 + h, yd.at[pl.ds(0, n), pl.ds(4 * h, 4)])

    @pl.when(me == 0)
    def _():
        drained(62)

    @pl.when((me > 0) & near0)
    def _():
        drained(61)

    @pl.when((me > 0) & jnp.logical_not(near0))
    def _():
        drained(63)

    @pl.when(me == 32)
    def _():
        wait_send(8, yq)

    for h in range(2):
        wait_send(3 + h, y2.at[pl.ds(0, H), pl.ds(4 * h, 4)])
        wait_send(5 + h, y3.at[pl.ds(0, H), pl.ds(4 * h, 4)])
    wait_send(7, y4.at[pl.ds(0, H)])
    wait_recv(7, out_h.at[:, pl.ds(0, H)])
    own4.wait()


def local(signal, gate_values, skip_gain, filter_spectrum):
    blocks, inner = make_tables()
    any_ = pl.BlockSpec(memory_space=pl.ANY)
    hbm = pl.BlockSpec(memory_space=pltpu.HBM)
    V = pltpu.VMEM
    dma = pltpu.SemaphoreType.DMA
    out = pl.pallas_call(
        kernel,
        out_shape=jax.ShapeDtypeStruct((16, 64, 8, 128), BF),
        in_specs=[hbm, hbm, hbm, hbm],
        out_specs=any_,
        scratch_shapes=[
            V((64, 16, 8, 128), BF),
            V((2, 8, 128, 8, 128), BF),
            V((64, 8, 16, 128), BF),
            V((64, 8, 16, 128), BF),
            V((16, 128), BF),
            V((8, 64, 16, 128), BF),
            V((64, 8, 16, 128), BF),
            V((64, 8, 16, 128), BF),
            V((64, 8, 16, 128), BF),
            V((64, 16, 8, 128), BF),
            V((64, 16, 1024), BF),
            V((64, 16, 1024), BF),
            V((64, 16, 1024), BF),
            V((64, 16, 1024), BF),
            V((64, 16, 1024), BF),
            V((64, 16, 8, 128), F32),
            V((8, 64, 16, 128), BF),
            V((16, 128), BF),
            V((1024, 1024), BF),
            V((1024, 128), F32),
            V((256, 1024), F32),
            V((1024, 512), BF),
            V((1024, 1024), F32),
            V((5, 2, N, 128), F32),
            V((6, 2, 16, 1024), F32),
            dma((9,)),
            dma((12,)),
            dma((12,)),
        ],
        compiler_params=pltpu.CompilerParams(
            collective_id=0, has_side_effects=True, vmem_limit_bytes=58 << 20
        ),
    )(
        signal.reshape(16, 64, 8, 128),
        filter_spectrum.reshape(2, 8, 128, 8, 128),
        jnp.asarray(blocks),
        jnp.asarray(inner),
    )
    grid = (16, 64, 8, 128)
    skipped = skip_gain * signal.reshape(grid).astype(F32)
    result = gate_values.reshape(grid).astype(F32) * (out.astype(F32) + skipped)
    return result.astype(BF).reshape(8192, 128)


def solution(mesh):
    return jax.shard_map(
        local,
        mesh=mesh,
        in_specs=(P("seq", "chan"), P("seq", "chan"), P("chan"), P(None, "seq", None, "chan")),
        out_specs=P("seq", "chan"),
        check_vma=False,
    )
```

```python
import math

import jax
import jax.numpy as jnp
import numpy as np
from jax import lax
from jax.experimental import pallas as pl
from jax.experimental.pallas import tpu as pltpu
from jax.sharding import PartitionSpec as P

MESH = pl.DeviceIdType.MESH
N = 64
H = N - 1
MULT = 37
OUTER = 1024
INNER = 512
SEQ = OUTER * INNER
BF = jnp.bfloat16
F32 = jnp.float32
SCALE = 1.0 / SEQ


def _circle(index, length):
    angle = 2.0 * np.pi / length * (index % length)
    return np.cos(angle), np.sin(angle)


def make_tables():
    pi = np.pi
    rows = np.arange(N)[:, None]
    lane = np.arange(128)[None, :]
    q = np.arange(16)[:, None]
    ro, x8 = q // 8, q % 8
    col = np.arange(1024)[None, :]
    a1 = 2 * pi / 128 * (rows * lane % 128)
    b1 = 2 * pi / 1024 * (x8 * col % 1024) + ro * pi / 2
    x = lane // 16 * 8 + lane % 8
    a2 = 2 * pi / 64 * (rows * x % 64)
    y = col // 16 * 8 + col % 8
    ri = col // 8 % 2
    b2 = 2 * pi / 512 * (x8 * y % 512) + (ro - ri) * pi / 2
    hh, u, c4, r4 = col // 512, col // 8 % 64, col // 2 % 4, col % 2
    c = 8 * u + 4 * hh + c4
    a4 = [2 * pi / 64 * (rows * c[:, h * 512 : h * 512 + 128] % 64) for h in range(2)]
    b4 = 2 * pi / 1024 * (q * c % 1024) + r4 * pi / 2
    half = 2 * pi / 1024 * y
    lo = (ri == 0) * np.ones((16, 1))
    hi = (ri == 1) * np.ones((16, 1))
    b2hi = b2 + ri * (pi / 2 + half)
    a3 = a2 + pi / 64 * rows
    up = col >= 512
    b3 = b2 + up * (pi / 1024 * 2 * x8 + pi)
    b3 = b3 - up * ro * pi / 2 + 0.0
    w3 = 2.0 * np.where(up, ro == 1, ro == 0)
    f = lambda m, w=1.0: np.stack([np.cos(m) * w, np.sin(m) * w])
    blocks = np.stack([f(a1), f(a2), f(a3), f(a4[0]), f(a4[1])])
    inner = np.stack(
        [f(b1), f(b2), f(b2, lo), f(b2hi, hi), f(b3, w3), f(b4, 2.0)]
    )
    return blocks.astype(np.float32), inner.astype(np.float32)


def peer(me, k):
    k = lax.rem(k * MULT, N)
    return (
        lax.rem(me // 16 + k // 16, 4) * 16
        + lax.rem(me // 4 + k // 4, 4) * 4
        + lax.rem(me // 2 + k // 2, 2) * 2
        + lax.rem(me + k, 2)
    )


def near(me, u):
    def gap(i, j):
        d = lax.rem(j - i + 4, 4)
        return jnp.minimum(d, 4 - d)

    def closer(i, j):
        return jnp.minimum(jnp.maximum(gap(3 - i, j) - gap(i, j), 0), 1)

    x = closer(me // 16, u // 16)
    z = closer(lax.rem(me // 4, 4), lax.rem(u // 4, 4))
    y = 1 - lax.rem(me // 2 + u // 2, 2)
    return x + z + y >= 2


def dot(x, y):
    return jnp.dot(x, y, preferred_element_type=F32)


def loop(n, body, start=0):
    def step(i, carry):
        body(i)
        return carry

    lax.fori_loop(start, n, step, 0)


def kernel(
    sig_h, filt_h, blk_h, inn_h, out_h,
    x1, fv, yd, ym, yq, x2, x4, y2, y3, y4,
    t1, t2, t2s, t3s, t4, wb, fw, nyq, xb, tr, acc, prod, part, blk, inn,
    ss, rs, ls,
):
    me = lax.axis_index("seq")
    ch = lax.axis_index("chan")
    bar = pltpu.get_barrier_semaphore()

    def hello(k):
        pl.semaphore_signal(bar, inc=1, device_id=(peer(me, k), ch), device_id_type=MESH)

    blk_in = pltpu.make_async_copy(blk_h, blk, ls.at[2])
    inn_in = pltpu.make_async_copy(inn_h, inn, ls.at[3])
    blk_in.start()
    inn_in.start()
    fv_in = pltpu.make_async_copy(filt_h, fv, ls.at[1])
    fv_in.start()
    loop(N, hello, 1)
    pl.semaphore_wait(bar, H)

    def remote(src, dst, s, r, p):
        return pltpu.make_async_remote_copy(
            src, dst, ss.at[s], rs.at[r], device_id=(p, ch), device_id_type=MESH
        )

    def wait_recv(r, ref):
        remote(ref, ref, 0, r, me).wait_recv()

    def wait_send(s, ref):
        remote(ref, ref, s, 0, me).wait_send()

    def copy(src, dst, s):
        return pltpu.make_async_copy(src, dst, ls.at[s])

    def send1(k):
        p = peer(me, k)
        remote(sig_h.at[:, p], x1.at[me], 0, 0, p).start()

    loop(N, send1, 1)
    own1 = copy(sig_h.at[:, me], x1.at[me], 0)
    own1.start()

    special = 1 - jnp.minimum(me, 1)
    row = lax.broadcasted_iota(jnp.int32, (16, 128), 0)
    lanes = lax.broadcasted_iota(jnp.int32, (16, 128), 1)

    def factors(i, p):
        return blk[i, 0, pl.ds(p, 1), :], blk[i, 1, pl.ds(p, 1), :]

    def tables(k):
        p = peer(me, k)
        a1 = factors(0, p)
        a2 = factors(1, p)
        a3 = factors(1 + special, p)
        a4 = (factors(3, p), factors(4, p))
        fwd = 1 + special * (1 + p // 32)
        inv = 1 + special * 3
        for j in range(8):
            cols = slice(j * 128, (j + 1) * 128)
            v = a1[0] * inn[0, 0, :, cols] - a1[1] * inn[0, 1, :, cols]
            alt = (1 - 2 * (lanes % 2)).astype(F32)
            v = jnp.where((row == 8) & (p == 0), alt, v)
            t1[k, :, cols] = v.astype(BF)
            v = a2[0] * inn[1, 0, :, cols] - a2[1] * inn[1, 1, :, cols]
            t2[k, :, cols] = v.astype(BF)
            v = a2[0] * inn[fwd, 0, :, cols] - a2[1] * inn[fwd, 1, :, cols]
            real = lanes // 8 % 2 == 0
            v = jnp.where((row == 8) & (p == 0) & (me == 0), jnp.where(real, alt, 0.0), v)
            t2s[k, :, cols] = v.astype(BF)
            a = a2 if j < 4 else a3
            v = a[0] * inn[inv, 0, :, cols] - a[1] * inn[inv, 1, :, cols]
            if j == 0:
                d0 = jnp.where(row < 8, jnp.where(lanes == 0, 1.0, (2 * (row % 2) - 1).astype(F32)), 0.0)
                v = jnp.where(((lanes == 0) | (lanes == 8)) & (me == 0), d0, v)
            t3s[k, :, cols] = v.astype(BF)
            a = a4[j // 4]
            v = a[0] * inn[5, 0, :, cols] - a[1] * inn[5, 1, :, cols]
            if j == 0:
                v = jnp.where(lanes == 0, 1.0, v)
                v = jnp.where(lanes == 1, (1 - 2 * (row % 2)).astype(F32), v)
            t4[k, :, cols] = v.astype(BF)

    blk_in.wait()
    inn_in.wait()
    loop(N, tables)

    fv_in.wait()
    sign = jnp.where(lax.broadcasted_iota(jnp.int32, (16, 128), 0) < 8, 1.0, -1.0)

    def direct(u):
        tr[0:128, :] = fv[:, :, u].astype(F32).reshape(128, 128)
        for c in range(8):
            yd[u, c] = tr[pl.ds(c, 16, stride=8), :].astype(BF)

    def mirrored(u):
        for p in range(2):
            for d in range(8):
                r = 128 + p * 64 + (7 - d) * 8
                tr[r : r + 8, :] = fv[p, d, 127 - u].astype(F32)
                tr[r + 128 : r + 136, :] = fv[p, d, 128 - u].astype(F32)
        ym[u, 0] = (tr[pl.ds(256, 16, stride=8), :] * sign).astype(BF)
        for c in range(1, 8):
            ym[u, c] = (tr[pl.ds(136 - c, 16, stride=8), :] * sign).astype(BF)

    def send_d(u, h):
        remote(
            yd.at[u, pl.ds(4 * h, 4)], fw.at[pl.ds(4 * h, 4), me], 1 + h, 1 + 10 * h, u
        ).start()

    def send_m(u, h):
        remote(
            ym.at[u, pl.ds(4 * h, 4)], fw.at[pl.ds(4 * h, 4), H - me], 1 + h, 1 + 10 * h, u
        ).start()

    direct(0)

    @pl.when(me >= 32)
    def _():
        tr[0:128, :] = fv[:, :, N].astype(F32).reshape(128, 128)
        yq[...] = yd[0, 0]
        yd[0, 0] = tr[pl.ds(0, 16, stride=8), :].astype(BF)

    @pl.when(me == 32)
    def _():
        remote(yq, nyq, 8, 2, 0).start()

    @pl.when(me > 0)
    def _():
        send_d(0, 0)

    def prepare(k):
        u = peer(me, k)

        @pl.when((u > 0) & near(me, u))
        def _():
            direct(u)
            mirrored(u)

            @pl.when(k > 0)
            def _():
                send_d(u, 0)
                send_m(u, 0)
                send_d(u, 1)
                send_m(u, 1)

    loop(N, prepare)

    def spread(u):
        r8 = lax.broadcasted_iota(jnp.int32, (8, 128), 0)
        l8 = lax.broadcasted_iota(jnp.int32, (8, 128), 1)
        turn = ((u * 8 + r8) * (me * 8 + l8 % 8)).astype(F32) * (2.0 * math.pi / SEQ)
        w = jnp.cos(turn - (l8 // 8).astype(F32) * (math.pi / 2))
        for j in range(16):
            wb[u, j] = jnp.broadcast_to(w[:, j : j + 1], (8, 128))

    loop(N, spread)

    wait_recv(0, x1.at[pl.ds(0, H)])
    own1.wait()

    def relay1(i):
        v = x1[pl.ds(i * 8, 8)].astype(F32).reshape(1024, 128)
        tr[...] = v
        for b in range(8):
            xb[pl.ds(pl.multiple_of(i * 128, 128), 128), b * 128 : (b + 1) * 128] = tr[
                pl.ds(b, 128, stride=8), :
            ].astype(BF)

    loop(8, relay1)

    for j in range(4):
        cols = slice(j * 256, (j + 1) * 256)
        part[:, cols] = dot(t1[...].reshape(1024, 1024), xb[:, cols])

    def stage1(g):

        def send2(i):
            k = g * 16 + i
            p = peer(me, k)

            @pl.when((k > 0) & (i >= 0))
            def _():
                remote(y2.at[k, pl.ds(0, 4)], x2.at[pl.ds(0, 4), me], 3, 3, p).start()

        def twist(i):
            k = g * 16 + i
            u = peer(me, k)
            r0 = pl.multiple_of(k * 16, 16)
            base = 0
            for b in range(8):
                re = part[pl.ds(r0, 8), b * 128 : (b + 1) * 128]
                im = part[pl.ds(r0 + 8, 8), b * 128 : (b + 1) * 128]
                wc = wb[u, b]
                ws = wb[u, 8 + b]
                tr[pl.ds(base + b, 8, stride=16), :] = re * wc + im * ws
                tr[pl.ds(base + 8 + b, 8, stride=16), :] = im * wc - re * ws
            y2[k] = tr[0:128, :].reshape(8, 16, 128).astype(BF)
            send2(i - 1)

        loop(16, twist)
        send2(15)

    loop(4, stage1)

    for j in range(8):
        x2[j, me] = y2[0, j]

    def send2b(k):
        p = peer(me, k)
        remote(y2.at[k, pl.ds(4, 4)], x2.at[pl.ds(4, 4), me], 4, 4, p).start()

    loop(N, send2b, 1)

    @pl.when(me > 0)
    def _():
        send_d(0, 1)

    for c in range(8):
        fw[c, me] = yd[me, c]

    @pl.when(me > 0)
    def _():
        for c in range(8):
            fw[c, H - me] = ym[me, c]

    @pl.when(me == 0)
    def _():
        wait_recv(2, nyq)

    for h in range(2):
        wait_recv(3 + h, x2.at[pl.ds(4 * h, 4), pl.ds(0, H)])

        @pl.when(me == 0)
        def _():
            wait_recv(1 + 10 * h, fw.at[pl.ds(4 * h, 4), pl.ds(0, N - 1)])

        @pl.when(me > 0)
        def _():
            wait_recv(1 + 10 * h, fw.at[pl.ds(4 * h, 4), pl.ds(0, N - 2)])

        cols = [x2[4 * h + j].reshape(1024, 128) for j in range(4)]
        for j in range(4):
            xb[:, j * 128 : (j + 1) * 128] = cols[j]

        def inner(first, ref, at):
            tab = t2[...].reshape(1024, 1024)
            if h == 0:
                part[:, at : at + 128] = dot(first[...].reshape(1024, 1024), ref[:, 0:128])
                part[:, at + 128 : at + 256] = dot(tab, ref[:, 128:256])
            else:
                part[:, at : at + 256] = dot(tab, ref[:, 0:256])
            part[:, at + 256 : at + 512] = dot(tab, ref[:, 256:512])

        inner(t2s, xb, 0)

        def stage2(g):
            def multiply(i):
                v = peer(me, g * 16 + i)
                r0 = pl.multiple_of(g * 256 + i * 16, 16)
                for j in range(4):
                    sr = part[pl.ds(r0, 8), j * 128 : (j + 1) * 128]
                    si = part[pl.ds(r0 + 8, 8), j * 128 : (j + 1) * 128]
                    f = fw[4 * h + j, v].astype(F32)
                    fre = f[0:8]
                    fim = f[8:16]
                    pr = sr * fre - si * fim
                    pi = -(sr * fim + si * fre)
                    prod[pl.ds(pl.multiple_of(v * 16, 16), 16), j * 128 : (j + 1) * 128] = (
                        jnp.concatenate([pr, pi], axis=0).astype(BF)
                    )

            loop(16, multiply)
            if h == 0:

                @pl.when((me == 0) & (g == 0))
                def _():
                    sr = part[0:8, 0:128]
                    si = part[8:16, 0:128]
                    f = fw[0, 0].astype(F32)
                    fre = f[0:8]
                    fim = f[8:16]
                    rows = lax.broadcasted_iota(jnp.int32, (8, 128), 0)
                    pr = sr * fre - si * fim
                    pi = -(sr * fim + si * fre)
                    pr = jnp.where(rows == 0, sr * fre, pr)
                    pi = jnp.where(rows == 0, -(si * nyq[...].astype(F32)[0:8]), pi)
                    prod[0:16, 0:128] = jnp.concatenate([pr, pi], axis=0).astype(BF)

        loop(4, stage2)

        inner(t3s, prod, 512)

        def stage3(g):
            def send3(i):
                k = g * 16 + i
                p = peer(me, k)

                @pl.when((k > 0) & (i >= 0))
                def _():
                    remote(
                        y3.at[k, pl.ds(4 * h, 4)], x4.at[me, pl.ds(4 * h, 4)], 5 + h, 5 + h, p
                    ).start()

            def untwist(i):
                k = g * 16 + i
                t = peer(me, k)
                r0 = pl.multiple_of(k * 16, 16)
                for j in range(4):
                    re = part[pl.ds(r0, 8), 512 + j * 128 : 640 + j * 128]
                    im = part[pl.ds(r0 + 8, 8), 512 + j * 128 : 640 + j * 128]
                    wc = wb[t, 4 * h + j]
                    ws = wb[t, 8 + 4 * h + j]
                    y3[k, 4 * h + j] = jnp.concatenate(
                        [re * wc + im * ws, re * ws - im * wc], axis=0
                    ).astype(BF)
                send3(i - 1)

            loop(16, untwist)
            send3(15)

        loop(4, stage3)
        for j in range(4):
            x4[me, 4 * h + j] = y3[0, 4 * h + j]

    for h in range(2):
        wait_recv(5 + h, x4.at[pl.ds(0, H), pl.ds(4 * h, 4)])

        def relay4(i):
            v = x4[pl.ds(i * 2, 2), 4 * h : 4 * h + 4].astype(F32).reshape(128, 128)
            tr[0:128, :] = v
            for b in range(8):
                xb[pl.ds(pl.multiple_of(h * 512 + i * 16, 16), 16), b * 128 : (b + 1) * 128] = tr[
                    pl.ds(b, 16, stride=8), :
                ].astype(BF)

        loop(32, relay4)

        def stage4(g):
            rows = pl.ds(pl.multiple_of(g * 256, 256), 256)
            acc[...] = part[rows, :] + dot(
                t4[pl.ds(g * 16, 16), :, 512:1024].reshape(256, 512), xb[512:1024, :]
            )

            def send4(i):
                k = g * 16 + i
                p = peer(me, k)

                @pl.when((k > 0) & (i >= 0))
                def _():
                    remote(y4.at[k], out_h.at[:, me], 7, 7, p).start()

            def finish(i):
                k = g * 16 + i
                r0 = pl.multiple_of(i * 16, 16)
                for b in range(8):
                    tr[pl.ds(b, 16, stride=8), :] = acc[pl.ds(r0, 16), b * 128 : (b + 1) * 128]
                y4[k] = (tr[0:128, :] * SCALE).reshape(16, 8, 128).astype(BF)
                send4(i - 1)

            loop(16, finish)
            send4(15)

        if h == 0:
            for j in range(4):
                cols = slice(j * 256, (j + 1) * 256)
                part[:, cols] = dot(t4[:, :, 0:512].reshape(1024, 512), xb[0:512, cols])
        else:
            loop(4, stage4)

    own4 = copy(y4.at[0], out_h.at[:, me], 10)
    own4.start()
    wait_send(0, sig_h.at[:, pl.ds(0, H)])
    near0 = near(me, 0)

    def drained(n):
        for h in range(2):
            wait_send(1 + h, yd.at[pl.ds(0, n), pl.ds(4 * h, 4)])

    @pl.when(me == 0)
    def _():
        drained(62)

    @pl.when((me > 0) & near0)
    def _():
        drained(61)

    @pl.when((me > 0) & jnp.logical_not(near0))
    def _():
        drained(63)

    @pl.when(me == 32)
    def _():
        wait_send(8, yq)

    for h in range(2):
        wait_send(3 + h, y2.at[pl.ds(0, H), pl.ds(4 * h, 4)])
        wait_send(5 + h, y3.at[pl.ds(0, H), pl.ds(4 * h, 4)])
    wait_send(7, y4.at[pl.ds(0, H)])
    wait_recv(7, out_h.at[:, pl.ds(0, H)])
    own4.wait()


def local(signal, gate_values, skip_gain, filter_spectrum):
    blocks, inner = make_tables()
    any_ = pl.BlockSpec(memory_space=pl.ANY)
    hbm = pl.BlockSpec(memory_space=pltpu.HBM)
    V = pltpu.VMEM
    dma = pltpu.SemaphoreType.DMA
    out = pl.pallas_call(
        kernel,
        out_shape=jax.ShapeDtypeStruct((16, 64, 8, 128), BF),
        in_specs=[hbm, hbm, hbm, hbm],
        out_specs=any_,
        scratch_shapes=[
            V((64, 16, 8, 128), BF),
            V((2, 8, 128, 8, 128), BF),
            V((64, 8, 16, 128), BF),
            V((64, 8, 16, 128), BF),
            V((16, 128), BF),
            V((8, 64, 16, 128), BF),
            V((64, 8, 16, 128), BF),
            V((64, 8, 16, 128), BF),
            V((64, 8, 16, 128), BF),
            V((64, 16, 8, 128), BF),
            V((64, 16, 1024), BF),
            V((64, 16, 1024), BF),
            V((64, 16, 1024), BF),
            V((64, 16, 1024), BF),
            V((64, 16, 1024), BF),
            V((64, 16, 8, 128), F32),
            V((8, 64, 16, 128), BF),
            V((16, 128), BF),
            V((1024, 1024), BF),
            V((1024, 128), F32),
            V((256, 1024), F32),
            V((1024, 512), BF),
            V((1024, 1024), F32),
            V((5, 2, N, 128), F32),
            V((6, 2, 16, 1024), F32),
            dma((9,)),
            dma((12,)),
            dma((12,)),
        ],
        compiler_params=pltpu.CompilerParams(
            collective_id=0, has_side_effects=True, vmem_limit_bytes=58 << 20
        ),
    )(
        signal.reshape(16, 64, 8, 128),
        filter_spectrum.reshape(2, 8, 128, 8, 128),
        jnp.asarray(blocks),
        jnp.asarray(inner),
    )
    grid = (16, 64, 8, 128)
    skipped = skip_gain * signal.reshape(grid).astype(F32)
    result = gate_values.reshape(grid).astype(F32) * (out.astype(F32) + skipped)
    return result.astype(BF).reshape(8192, 128)


def solution(mesh):
    return jax.shard_map(
        local,
        mesh=mesh,
        in_specs=(P("seq", "chan"), P("seq", "chan"), P("chan"), P(None, "seq", None, "chan")),
        out_specs=P("seq", "chan"),
        check_vma=False,
    )
```

```python
import math

import jax
import jax.numpy as jnp
import numpy as np
from jax import lax
from jax.experimental import pallas as pl
from jax.experimental.pallas import tpu as pltpu
from jax.sharding import PartitionSpec as P

MESH = pl.DeviceIdType.MESH
N = 64
H = N - 1
MULT = 37
OUTER = 1024
INNER = 512
SEQ = OUTER * INNER
BF = jnp.bfloat16
F32 = jnp.float32
SCALE = 1.0 / SEQ


def _circle(index, length):
    angle = 2.0 * np.pi / length * (index % length)
    return np.cos(angle), np.sin(angle)


def make_tables():
    pi = np.pi
    rows = np.arange(N)[:, None]
    lane = np.arange(128)[None, :]
    q = np.arange(16)[:, None]
    ro, x8 = q // 8, q % 8
    col = np.arange(1024)[None, :]
    a1 = 2 * pi / 128 * (rows * lane % 128)
    b1 = 2 * pi / 1024 * (x8 * col % 1024) + ro * pi / 2
    x = lane // 16 * 8 + lane % 8
    a2 = 2 * pi / 64 * (rows * x % 64)
    y = col // 16 * 8 + col % 8
    ri = col // 8 % 2
    b2 = 2 * pi / 512 * (x8 * y % 512) + (ro - ri) * pi / 2
    hh, u, c4, r4 = col // 512, col // 8 % 64, col // 2 % 4, col % 2
    c = 8 * u + 4 * hh + c4
    a4 = [2 * pi / 64 * (rows * c[:, h * 512 : h * 512 + 128] % 64) for h in range(2)]
    b4 = 2 * pi / 1024 * (q * c % 1024) + r4 * pi / 2
    half = 2 * pi / 1024 * y
    lo = (ri == 0) * np.ones((16, 1))
    hi = (ri == 1) * np.ones((16, 1))
    b2hi = b2 + ri * (pi / 2 + half)
    a3 = a2 + pi / 64 * rows
    up = col >= 512
    b3 = b2 + up * (pi / 1024 * 2 * x8 + pi)
    b3 = b3 - up * ro * pi / 2 + 0.0
    w3 = 2.0 * np.where(up, ro == 1, ro == 0)
    f = lambda m, w=1.0: np.stack([np.cos(m) * w, np.sin(m) * w])
    blocks = np.stack([f(a1), f(a2), f(a3), f(a4[0]), f(a4[1])])
    inner = np.stack(
        [f(b1), f(b2), f(b2, lo), f(b2hi, hi), f(b3, w3), f(b4, 2.0)]
    )
    return blocks.astype(np.float32), inner.astype(np.float32)


def peer(me, k):
    k = lax.rem(k * MULT, N)
    return (
        lax.rem(me // 16 + k // 16, 4) * 16
        + lax.rem(me // 4 + k // 4, 4) * 4
        + lax.rem(me // 2 + k // 2, 2) * 2
        + lax.rem(me + k, 2)
    )


def near(me, u):
    def gap(i, j):
        d = lax.rem(j - i + 4, 4)
        return jnp.minimum(d, 4 - d)

    def closer(i, j):
        return jnp.minimum(jnp.maximum(gap(3 - i, j) - gap(i, j), 0), 1)

    x = closer(me // 16, u // 16)
    z = closer(lax.rem(me // 4, 4), lax.rem(u // 4, 4))
    y = 1 - lax.rem(me // 2 + u // 2, 2)
    return x + z + y >= 2


def dot(x, y):
    return jnp.dot(x, y, preferred_element_type=F32)


def loop(n, body, start=0):
    def step(i, carry):
        body(i)
        return carry

    lax.fori_loop(start, n, step, 0)


def kernel(
    sig_h, filt_h, blk_h, inn_h, out_h,
    x1, fv, yd, ym, yq, x2, x4, y2, y3, y4,
    t1, t2, t2s, t3s, t4, wb, fw, nyq, xb, tr, acc, prod, part, blk, inn,
    ss, rs, ls,
):
    me = lax.axis_index("seq")
    ch = lax.axis_index("chan")
    bar = pltpu.get_barrier_semaphore()

    def hello(k):
        pl.semaphore_signal(bar, inc=1, device_id=(peer(me, k), ch), device_id_type=MESH)

    blk_in = pltpu.make_async_copy(blk_h, blk, ls.at[2])
    inn_in = pltpu.make_async_copy(inn_h, inn, ls.at[3])
    blk_in.start()
    inn_in.start()
    fv_in = pltpu.make_async_copy(filt_h, fv, ls.at[1])
    fv_in.start()
    loop(N, hello, 1)
    pl.semaphore_wait(bar, H)

    def remote(src, dst, s, r, p):
        return pltpu.make_async_remote_copy(
            src, dst, ss.at[s], rs.at[r], device_id=(p, ch), device_id_type=MESH
        )

    def wait_recv(r, ref):
        remote(ref, ref, 0, r, me).wait_recv()

    def wait_send(s, ref):
        remote(ref, ref, s, 0, me).wait_send()

    def copy(src, dst, s):
        return pltpu.make_async_copy(src, dst, ls.at[s])

    def send1(k):
        p = peer(me, k)
        remote(sig_h.at[:, p], x1.at[me], 0, 0, p).start()

    loop(N, send1, 1)
    own1 = copy(sig_h.at[:, me], x1.at[me], 0)
    own1.start()

    special = 1 - jnp.minimum(me, 1)
    row = lax.broadcasted_iota(jnp.int32, (16, 128), 0)
    lanes = lax.broadcasted_iota(jnp.int32, (16, 128), 1)

    def factors(i, p):
        return blk[i, 0, pl.ds(p, 1), :], blk[i, 1, pl.ds(p, 1), :]

    def tables(k):
        p = peer(me, k)
        a1 = factors(0, p)
        a2 = factors(1, p)
        a3 = factors(1 + special, p)
        a4 = (factors(3, p), factors(4, p))
        fwd = 1 + special * (1 + p // 32)
        inv = 1 + special * 3
        for j in range(8):
            cols = slice(j * 128, (j + 1) * 128)
            v = a1[0] * inn[0, 0, :, cols] - a1[1] * inn[0, 1, :, cols]
            alt = (1 - 2 * (lanes % 2)).astype(F32)
            v = jnp.where((row == 8) & (p == 0), alt, v)
            t1[k, :, cols] = v.astype(BF)
            v = a2[0] * inn[1, 0, :, cols] - a2[1] * inn[1, 1, :, cols]
            t2[k, :, cols] = v.astype(BF)
            v = a2[0] * inn[fwd, 0, :, cols] - a2[1] * inn[fwd, 1, :, cols]
            real = lanes // 8 % 2 == 0
            v = jnp.where((row == 8) & (p == 0) & (me == 0), jnp.where(real, alt, 0.0), v)
            t2s[k, :, cols] = v.astype(BF)
            a = a2 if j < 4 else a3
            v = a[0] * inn[inv, 0, :, cols] - a[1] * inn[inv, 1, :, cols]
            if j == 0:
                d0 = jnp.where(row < 8, jnp.where(lanes == 0, 1.0, (2 * (row % 2) - 1).astype(F32)), 0.0)
                v = jnp.where(((lanes == 0) | (lanes == 8)) & (me == 0), d0, v)
            t3s[k, :, cols] = v.astype(BF)
            a = a4[j // 4]
            v = a[0] * inn[5, 0, :, cols] - a[1] * inn[5, 1, :, cols]
            if j == 0:
                v = jnp.where(lanes == 0, 1.0, v)
                v = jnp.where(lanes == 1, (1 - 2 * (row % 2)).astype(F32), v)
            t4[k, :, cols] = v.astype(BF)

    blk_in.wait()
    inn_in.wait()
    loop(N, tables)

    fv_in.wait()
    sign = jnp.where(lax.broadcasted_iota(jnp.int32, (16, 128), 0) < 8, 1.0, -1.0)

    def direct(u):
        tr[0:128, :] = fv[:, :, u].astype(F32).reshape(128, 128)
        for c in range(8):
            yd[u, c] = tr[pl.ds(c, 16, stride=8), :].astype(BF)

    def mirrored(u):
        for p in range(2):
            for d in range(8):
                r = 128 + p * 64 + (7 - d) * 8
                tr[r : r + 8, :] = fv[p, d, 127 - u].astype(F32)
                tr[r + 128 : r + 136, :] = fv[p, d, 128 - u].astype(F32)
        ym[u, 0] = (tr[pl.ds(256, 16, stride=8), :] * sign).astype(BF)
        for c in range(1, 8):
            ym[u, c] = (tr[pl.ds(136 - c, 16, stride=8), :] * sign).astype(BF)

    def send_d(u, h):
        remote(
            yd.at[u, pl.ds(4 * h, 4)], fw.at[pl.ds(4 * h, 4), me], 1 + h, 1 + 10 * h, u
        ).start()

    def send_m(u, h):
        remote(
            ym.at[u, pl.ds(4 * h, 4)], fw.at[pl.ds(4 * h, 4), H - me], 1 + h, 1 + 10 * h, u
        ).start()

    direct(0)

    @pl.when(me >= 32)
    def _():
        tr[0:128, :] = fv[:, :, N].astype(F32).reshape(128, 128)
        yq[...] = yd[0, 0]
        yd[0, 0] = tr[pl.ds(0, 16, stride=8), :].astype(BF)

    @pl.when(me == 32)
    def _():
        remote(yq, nyq, 8, 2, 0).start()

    @pl.when(me > 0)
    def _():
        send_d(0, 0)

    def prepare(k):
        u = peer(me, k)

        @pl.when((u > 0) & near(me, u))
        def _():
            direct(u)
            mirrored(u)

            @pl.when(k > 0)
            def _():
                send_d(u, 0)
                send_m(u, 0)
                send_d(u, 1)
                send_m(u, 1)

    loop(N, prepare)

    def spread(u):
        r8 = lax.broadcasted_iota(jnp.int32, (8, 128), 0)
        l8 = lax.broadcasted_iota(jnp.int32, (8, 128), 1)
        turn = ((u * 8 + r8) * (me * 8 + l8 % 8)).astype(F32) * (2.0 * math.pi / SEQ)
        w = jnp.cos(turn - (l8 // 8).astype(F32) * (math.pi / 2))
        for j in range(16):
            wb[u, j] = jnp.broadcast_to(w[:, j : j + 1], (8, 128))

    loop(N, spread)

    wait_recv(0, x1.at[pl.ds(0, H)])
    own1.wait()

    def relay1(i):
        v = x1[pl.ds(i * 8, 8)].astype(F32).reshape(1024, 128)
        tr[0:1024, :] = v
        for b in range(8):
            xb[pl.ds(pl.multiple_of(i * 128, 128), 128), b * 128 : (b + 1) * 128] = tr[
                pl.ds(b, 128, stride=8), :
            ].astype(BF)

    loop(8, relay1)

    for j in range(4):
        cols = slice(j * 256, (j + 1) * 256)
        part[:, cols] = dot(t1[...].reshape(1024, 1024), xb[:, cols])

    def stage1(g):

        def send2(i):
            k = g * 16 + i
            p = peer(me, k)

            @pl.when((k > 0) & (i >= 0))
            def _():
                remote(y2.at[k, pl.ds(0, 4)], x2.at[pl.ds(0, 4), me], 3, 3, p).start()

        def twist(i):
            k = g * 16 + i
            u = peer(me, k)
            r0 = pl.multiple_of(k * 16, 16)
            base = 0
            for b in range(8):
                re = part[pl.ds(r0, 8), b * 128 : (b + 1) * 128]
                im = part[pl.ds(r0 + 8, 8), b * 128 : (b + 1) * 128]
                wc = wb[u, b]
                ws = wb[u, 8 + b]
                tr[pl.ds(base + b, 8, stride=16), :] = re * wc + im * ws
                tr[pl.ds(base + 8 + b, 8, stride=16), :] = im * wc - re * ws
            y2[k] = tr[0:128, :].reshape(8, 16, 128).astype(BF)
            send2(i - 1)

        loop(16, twist)
        send2(15)

    loop(4, stage1)

    for j in range(8):
        x2[j, me] = y2[0, j]

    def send2b(k):
        p = peer(me, k)
        remote(y2.at[k, pl.ds(4, 4)], x2.at[pl.ds(4, 4), me], 4, 4, p).start()

    loop(N, send2b, 1)

    @pl.when(me > 0)
    def _():
        send_d(0, 1)

    for c in range(8):
        fw[c, me] = yd[me, c]

    @pl.when(me > 0)
    def _():
        for c in range(8):
            fw[c, H - me] = ym[me, c]

    @pl.when(me == 0)
    def _():
        wait_recv(2, nyq)

    for h in range(2):
        wait_recv(3 + h, x2.at[pl.ds(4 * h, 4), pl.ds(0, H)])

        @pl.when(me == 0)
        def _():
            wait_recv(1 + 10 * h, fw.at[pl.ds(4 * h, 4), pl.ds(0, N - 1)])

        @pl.when(me > 0)
        def _():
            wait_recv(1 + 10 * h, fw.at[pl.ds(4 * h, 4), pl.ds(0, N - 2)])

        cols = [x2[4 * h + j].reshape(1024, 128) for j in range(4)]
        for j in range(4):
            xb[:, j * 128 : (j + 1) * 128] = cols[j]

        def inner(first, ref, at):
            tab = t2[...].reshape(1024, 1024)
            if h == 0:
                part[:, at : at + 128] = dot(first[...].reshape(1024, 1024), ref[:, 0:128])
                part[:, at + 128 : at + 256] = dot(tab, ref[:, 128:256])
            else:
                part[:, at : at + 256] = dot(tab, ref[:, 0:256])
            part[:, at + 256 : at + 512] = dot(tab, ref[:, 256:512])

        inner(t2s, xb, 0)

        def stage2(g):
            def multiply(i):
                v = peer(me, g * 16 + i)
                r0 = pl.multiple_of(g * 256 + i * 16, 16)
                for j in range(4):
                    sr = part[pl.ds(r0, 8), j * 128 : (j + 1) * 128]
                    si = part[pl.ds(r0 + 8, 8), j * 128 : (j + 1) * 128]
                    f = fw[4 * h + j, v].astype(F32)
                    fre = f[0:8]
                    fim = f[8:16]
                    pr = sr * fre - si * fim
                    pi = -(sr * fim + si * fre)
                    prod[pl.ds(pl.multiple_of(v * 16, 16), 16), j * 128 : (j + 1) * 128] = (
                        jnp.concatenate([pr, pi], axis=0).astype(BF)
                    )

            loop(16, multiply)
            if h == 0:

                @pl.when((me == 0) & (g == 0))
                def _():
                    sr = part[0:8, 0:128]
                    si = part[8:16, 0:128]
                    f = fw[0, 0].astype(F32)
                    fre = f[0:8]
                    fim = f[8:16]
                    rows = lax.broadcasted_iota(jnp.int32, (8, 128), 0)
                    pr = sr * fre - si * fim
                    pi = -(sr * fim + si * fre)
                    pr = jnp.where(rows == 0, sr * fre, pr)
                    pi = jnp.where(rows == 0, -(si * nyq[...].astype(F32)[0:8]), pi)
                    prod[0:16, 0:128] = jnp.concatenate([pr, pi], axis=0).astype(BF)

        loop(4, stage2)

        inner(t3s, prod, 512)

        def stage3(g):
            def send3(i):
                k = g * 16 + i
                p = peer(me, k)

                @pl.when((k > 0) & (i >= 0))
                def _():
                    remote(
                        y3.at[k, pl.ds(4 * h, 4)], x4.at[me, pl.ds(4 * h, 4)], 5 + h, 5 + h, p
                    ).start()

            def untwist(i):
                k = g * 16 + i
                t = peer(me, k)
                r0 = pl.multiple_of(k * 16, 16)
                for j in range(4):
                    re = part[pl.ds(r0, 8), 512 + j * 128 : 640 + j * 128]
                    im = part[pl.ds(r0 + 8, 8), 512 + j * 128 : 640 + j * 128]
                    wc = wb[t, 4 * h + j]
                    ws = wb[t, 8 + 4 * h + j]
                    y3[k, 4 * h + j] = jnp.concatenate(
                        [re * wc + im * ws, re * ws - im * wc], axis=0
                    ).astype(BF)
                send3(i - 1)

            loop(16, untwist)
            send3(15)

        loop(4, stage3)
        for j in range(4):
            x4[me, 4 * h + j] = y3[0, 4 * h + j]

    for h in range(2):
        wait_recv(5 + h, x4.at[pl.ds(0, H), pl.ds(4 * h, 4)])

        def relay4(i):
            v = x4[pl.ds(i * 2, 2), 4 * h : 4 * h + 4].astype(F32).reshape(128, 128)
            tr[0:128, :] = v
            for b in range(8):
                xb[pl.ds(pl.multiple_of(h * 512 + i * 16, 16), 16), b * 128 : (b + 1) * 128] = tr[
                    pl.ds(b, 16, stride=8), :
                ].astype(BF)

        loop(32, relay4)

        def stage4(g):
            rows = pl.ds(pl.multiple_of(g * 256, 256), 256)
            acc[...] = part[rows, :] + dot(
                t4[pl.ds(g * 16, 16), :, 512:1024].reshape(256, 512), xb[512:1024, :]
            )

            def send4(i):
                k = g * 16 + i
                p = peer(me, k)

                @pl.when((k > 0) & (i >= 0))
                def _():
                    remote(y4.at[k], out_h.at[:, me], 7, 7, p).start()

            def finish(i):
                k = g * 16 + i
                r0 = pl.multiple_of(i * 16, 16)
                for b in range(8):
                    tr[pl.ds(b, 16, stride=8), :] = acc[pl.ds(r0, 16), b * 128 : (b + 1) * 128]
                y4[k] = (tr[0:128, :] * SCALE).reshape(16, 8, 128).astype(BF)
                send4(i - 1)

            loop(16, finish)
            send4(15)

        if h == 0:
            for j in range(4):
                cols = slice(j * 256, (j + 1) * 256)
                part[:, cols] = dot(t4[:, :, 0:512].reshape(1024, 512), xb[0:512, cols])
        else:
            loop(4, stage4)

    own4 = copy(y4.at[0], out_h.at[:, me], 10)
    own4.start()
    wait_send(0, sig_h.at[:, pl.ds(0, H)])
    near0 = near(me, 0)

    def drained(n):
        for h in range(2):
            wait_send(1 + h, yd.at[pl.ds(0, n), pl.ds(4 * h, 4)])

    @pl.when(me == 0)
    def _():
        drained(62)

    @pl.when((me > 0) & near0)
    def _():
        drained(61)

    @pl.when((me > 0) & jnp.logical_not(near0))
    def _():
        drained(63)

    @pl.when(me == 32)
    def _():
        wait_send(8, yq)

    for h in range(2):
        wait_send(3 + h, y2.at[pl.ds(0, H), pl.ds(4 * h, 4)])
        wait_send(5 + h, y3.at[pl.ds(0, H), pl.ds(4 * h, 4)])
    wait_send(7, y4.at[pl.ds(0, H)])
    wait_recv(7, out_h.at[:, pl.ds(0, H)])
    own4.wait()


def local(signal, gate_values, skip_gain, filter_spectrum):
    blocks, inner = make_tables()
    any_ = pl.BlockSpec(memory_space=pl.ANY)
    hbm = pl.BlockSpec(memory_space=pltpu.HBM)
    V = pltpu.VMEM
    dma = pltpu.SemaphoreType.DMA
    out = pl.pallas_call(
        kernel,
        out_shape=jax.ShapeDtypeStruct((16, 64, 8, 128), BF),
        in_specs=[hbm, hbm, hbm, hbm],
        out_specs=any_,
        scratch_shapes=[
            V((64, 16, 8, 128), BF),
            V((2, 8, 128, 8, 128), BF),
            V((64, 8, 16, 128), BF),
            V((64, 8, 16, 128), BF),
            V((16, 128), BF),
            V((8, 64, 16, 128), BF),
            V((64, 8, 16, 128), BF),
            V((64, 8, 16, 128), BF),
            V((64, 8, 16, 128), BF),
            V((64, 16, 8, 128), BF),
            V((64, 16, 1024), BF),
            V((64, 16, 1024), BF),
            V((64, 16, 1024), BF),
            V((64, 16, 1024), BF),
            V((64, 16, 1024), BF),
            V((64, 16, 8, 128), F32),
            V((8, 64, 16, 128), BF),
            V((16, 128), BF),
            V((1024, 1024), BF),
            V((1152, 128), F32),
            V((256, 1024), F32),
            V((1024, 512), BF),
            V((1024, 1024), F32),
            V((5, 2, N, 128), F32),
            V((6, 2, 16, 1024), F32),
            dma((9,)),
            dma((12,)),
            dma((12,)),
        ],
        compiler_params=pltpu.CompilerParams(
            collective_id=0, has_side_effects=True, vmem_limit_bytes=58 << 20
        ),
    )(
        signal.reshape(16, 64, 8, 128),
        filter_spectrum.reshape(2, 8, 128, 8, 128),
        jnp.asarray(blocks),
        jnp.asarray(inner),
    )
    grid = (16, 64, 8, 128)
    skipped = skip_gain * signal.reshape(grid).astype(F32)
    result = gate_values.reshape(grid).astype(F32) * (out.astype(F32) + skipped)
    return result.astype(BF).reshape(8192, 128)


def solution(mesh):
    return jax.shard_map(
        local,
        mesh=mesh,
        in_specs=(P("seq", "chan"), P("seq", "chan"), P("chan"), P(None, "seq", None, "chan")),
        out_specs=P("seq", "chan"),
        check_vma=False,
    )
```

```python
import math

import jax
import jax.numpy as jnp
import numpy as np
from jax import lax
from jax.experimental import pallas as pl
from jax.experimental.pallas import tpu as pltpu
from jax.sharding import PartitionSpec as P

MESH = pl.DeviceIdType.MESH
N = 64
H = N - 1
MULT = 45
OUTER = 1024
INNER = 512
SEQ = OUTER * INNER
BF = jnp.bfloat16
F32 = jnp.float32
SCALE = 1.0 / SEQ


def _circle(index, length):
    angle = 2.0 * np.pi / length * (index % length)
    return np.cos(angle), np.sin(angle)


def make_tables():
    pi = np.pi
    rows = np.arange(N)[:, None]
    lane = np.arange(128)[None, :]
    q = np.arange(16)[:, None]
    ro, x8 = q // 8, q % 8
    col = np.arange(1024)[None, :]
    a1 = 2 * pi / 128 * (rows * lane % 128)
    b1 = 2 * pi / 1024 * (x8 * col % 1024) + ro * pi / 2
    x = lane // 16 * 8 + lane % 8
    a2 = 2 * pi / 64 * (rows * x % 64)
    y = col // 16 * 8 + col % 8
    ri = col // 8 % 2
    b2 = 2 * pi / 512 * (x8 * y % 512) + (ro - ri) * pi / 2
    hh, u, c4, r4 = col // 512, col // 8 % 64, col // 2 % 4, col % 2
    c = 8 * u + 4 * hh + c4
    a4 = [2 * pi / 64 * (rows * c[:, h * 512 : h * 512 + 128] % 64) for h in range(2)]
    b4 = 2 * pi / 1024 * (q * c % 1024) + r4 * pi / 2
    half = 2 * pi / 1024 * y
    lo = (ri == 0) * np.ones((16, 1))
    hi = (ri == 1) * np.ones((16, 1))
    b2hi = b2 + ri * (pi / 2 + half)
    a3 = a2 + pi / 64 * rows
    up = col >= 512
    b3 = b2 + up * (pi / 1024 * 2 * x8 + pi)
    b3 = b3 - up * ro * pi / 2 + 0.0
    w3 = 2.0 * np.where(up, ro == 1, ro == 0)
    f = lambda m, w=1.0: np.stack([np.cos(m) * w, np.sin(m) * w])
    blocks = np.stack([f(a1), f(a2), f(a3), f(a4[0]), f(a4[1])])
    inner = np.stack(
        [f(b1), f(b2), f(b2, lo), f(b2hi, hi), f(b3, w3), f(b4, 2.0)]
    )
    return blocks.astype(np.float32), inner.astype(np.float32)


def peer(me, k):
    k = lax.rem(k * MULT, N)
    return (
        lax.rem(me // 16 + k // 16, 4) * 16
        + lax.rem(me // 4 + k // 4, 4) * 4
        + lax.rem(me // 2 + k // 2, 2) * 2
        + lax.rem(me + k, 2)
    )


def near(me, u):
    def gap(i, j):
        d = lax.rem(j - i + 4, 4)
        return jnp.minimum(d, 4 - d)

    def closer(i, j):
        return jnp.minimum(jnp.maximum(gap(3 - i, j) - gap(i, j), 0), 1)

    x = closer(me // 16, u // 16)
    z = closer(lax.rem(me // 4, 4), lax.rem(u // 4, 4))
    y = 1 - lax.rem(me // 2 + u // 2, 2)
    return x + z + y >= 2


def dot(x, y):
    return jnp.dot(x, y, preferred_element_type=F32)


def loop(n, body, start=0):
    def step(i, carry):
        body(i)
        return carry

    lax.fori_loop(start, n, step, 0)


def kernel(
    sig_h, filt_h, blk_h, inn_h, out_h,
    x1, fv, yd, ym, yq, x2, x4, y2, y3, y4,
    t1, t2, t2s, t3s, t4, wb, fw, nyq, xb, tr, acc, prod, part, blk, inn,
    ss, rs, ls,
):
    me = lax.axis_index("seq")
    ch = lax.axis_index("chan")
    bar = pltpu.get_barrier_semaphore()

    def hello(k):
        pl.semaphore_signal(bar, inc=1, device_id=(peer(me, k), ch), device_id_type=MESH)

    blk_in = pltpu.make_async_copy(blk_h, blk, ls.at[2])
    inn_in = pltpu.make_async_copy(inn_h, inn, ls.at[3])
    blk_in.start()
    inn_in.start()
    fv_in = pltpu.make_async_copy(filt_h, fv, ls.at[1])
    fv_in.start()
    loop(N, hello, 1)
    pl.semaphore_wait(bar, H)

    def remote(src, dst, s, r, p):
        return pltpu.make_async_remote_copy(
            src, dst, ss.at[s], rs.at[r], device_id=(p, ch), device_id_type=MESH
        )

    def wait_recv(r, ref):
        remote(ref, ref, 0, r, me).wait_recv()

    def wait_send(s, ref):
        remote(ref, ref, s, 0, me).wait_send()

    def copy(src, dst, s):
        return pltpu.make_async_copy(src, dst, ls.at[s])

    def send1(k):
        p = peer(me, k)
        remote(sig_h.at[:, p], x1.at[me], 0, 0, p).start()

    loop(N, send1, 1)
    own1 = copy(sig_h.at[:, me], x1.at[me], 0)
    own1.start()

    special = 1 - jnp.minimum(me, 1)
    row = lax.broadcasted_iota(jnp.int32, (16, 128), 0)
    lanes = lax.broadcasted_iota(jnp.int32, (16, 128), 1)

    def factors(i, p):
        return blk[i, 0, pl.ds(p, 1), :], blk[i, 1, pl.ds(p, 1), :]

    def tables(k):
        p = peer(me, k)
        a1 = factors(0, p)
        a2 = factors(1, p)
        a3 = factors(1 + special, p)
        a4 = (factors(3, p), factors(4, p))
        fwd = 1 + special * (1 + p // 32)
        inv = 1 + special * 3
        for j in range(8):
            cols = slice(j * 128, (j + 1) * 128)
            v = a1[0] * inn[0, 0, :, cols] - a1[1] * inn[0, 1, :, cols]
            alt = (1 - 2 * (lanes % 2)).astype(F32)
            v = jnp.where((row == 8) & (p == 0), alt, v)
            t1[k, :, cols] = v.astype(BF)
            v = a2[0] * inn[1, 0, :, cols] - a2[1] * inn[1, 1, :, cols]
            t2[k, :, cols] = v.astype(BF)
            v = a2[0] * inn[fwd, 0, :, cols] - a2[1] * inn[fwd, 1, :, cols]
            real = lanes // 8 % 2 == 0
            v = jnp.where((row == 8) & (p == 0) & (me == 0), jnp.where(real, alt, 0.0), v)
            t2s[k, :, cols] = v.astype(BF)
            a = a2 if j < 4 else a3
            v = a[0] * inn[inv, 0, :, cols] - a[1] * inn[inv, 1, :, cols]
            if j == 0:
                d0 = jnp.where(row < 8, jnp.where(lanes == 0, 1.0, (2 * (row % 2) - 1).astype(F32)), 0.0)
                v = jnp.where(((lanes == 0) | (lanes == 8)) & (me == 0), d0, v)
            t3s[k, :, cols] = v.astype(BF)
            a = a4[j // 4]
            v = a[0] * inn[5, 0, :, cols] - a[1] * inn[5, 1, :, cols]
            if j == 0:
                v = jnp.where(lanes == 0, 1.0, v)
                v = jnp.where(lanes == 1, (1 - 2 * (row % 2)).astype(F32), v)
            t4[k, :, cols] = v.astype(BF)

    blk_in.wait()
    inn_in.wait()
    loop(N, tables)

    fv_in.wait()
    sign = jnp.where(lax.broadcasted_iota(jnp.int32, (16, 128), 0) < 8, 1.0, -1.0)

    def direct(u):
        tr[0:128, :] = fv[:, :, u].astype(F32).reshape(128, 128)
        for c in range(8):
            yd[u, c] = tr[pl.ds(c, 16, stride=8), :].astype(BF)

    def mirrored(u):
        for p in range(2):
            for d in range(8):
                r = 128 + p * 64 + (7 - d) * 8
                tr[r : r + 8, :] = fv[p, d, 127 - u].astype(F32)
                tr[r + 128 : r + 136, :] = fv[p, d, 128 - u].astype(F32)
        ym[u, 0] = (tr[pl.ds(256, 16, stride=8), :] * sign).astype(BF)
        for c in range(1, 8):
            ym[u, c] = (tr[pl.ds(136 - c, 16, stride=8), :] * sign).astype(BF)

    def send_d(u, h):
        remote(
            yd.at[u, pl.ds(4 * h, 4)], fw.at[pl.ds(4 * h, 4), me], 1 + h, 1 + 10 * h, u
        ).start()

    def send_m(u, h):
        remote(
            ym.at[u, pl.ds(4 * h, 4)], fw.at[pl.ds(4 * h, 4), H - me], 1 + h, 1 + 10 * h, u
        ).start()

    direct(0)

    @pl.when(me >= 32)
    def _():
        tr[0:128, :] = fv[:, :, N].astype(F32).reshape(128, 128)
        yq[...] = yd[0, 0]
        yd[0, 0] = tr[pl.ds(0, 16, stride=8), :].astype(BF)

    @pl.when(me == 32)
    def _():
        remote(yq, nyq, 8, 2, 0).start()

    @pl.when(me > 0)
    def _():
        send_d(0, 0)

    def prepare(k):
        u = peer(me, k)

        @pl.when((u > 0) & near(me, u))
        def _():
            direct(u)
            mirrored(u)

            @pl.when(k > 0)
            def _():
                send_d(u, 0)
                send_m(u, 0)
                send_d(u, 1)
                send_m(u, 1)

    loop(N, prepare)

    def spread(u):
        r8 = lax.broadcasted_iota(jnp.int32, (8, 128), 0)
        l8 = lax.broadcasted_iota(jnp.int32, (8, 128), 1)
        turn = ((u * 8 + r8) * (me * 8 + l8 % 8)).astype(F32) * (2.0 * math.pi / SEQ)
        w = jnp.cos(turn - (l8 // 8).astype(F32) * (math.pi / 2))
        for j in range(16):
            wb[u, j] = jnp.broadcast_to(w[:, j : j + 1], (8, 128))

    loop(N, spread)

    wait_recv(0, x1.at[pl.ds(0, H)])
    own1.wait()

    def relay1(i):
        v = x1[pl.ds(i * 8, 8)].astype(F32).reshape(1024, 128)
        tr[0:1024, :] = v
        for b in range(8):
            xb[pl.ds(pl.multiple_of(i * 128, 128), 128), b * 128 : (b + 1) * 128] = tr[
                pl.ds(b, 128, stride=8), :
            ].astype(BF)

    loop(8, relay1)

    for j in range(4):
        cols = slice(j * 256, (j + 1) * 256)
        part[:, cols] = dot(t1[...].reshape(1024, 1024), xb[:, cols])

    def stage1(g):

        def send2(i):
            k = g * 16 + i
            p = peer(me, k)

            @pl.when((k > 0) & (i >= 0))
            def _():
                remote(y2.at[k, pl.ds(0, 4)], x2.at[pl.ds(0, 4), me], 3, 3, p).start()

        def twist(i):
            k = g * 16 + i
            u = peer(me, k)
            r0 = pl.multiple_of(k * 16, 16)
            base = 0
            for b in range(8):
                re = part[pl.ds(r0, 8), b * 128 : (b + 1) * 128]
                im = part[pl.ds(r0 + 8, 8), b * 128 : (b + 1) * 128]
                wc = wb[u, b]
                ws = wb[u, 8 + b]
                tr[pl.ds(base + b, 8, stride=16), :] = re * wc + im * ws
                tr[pl.ds(base + 8 + b, 8, stride=16), :] = im * wc - re * ws
            y2[k] = tr[0:128, :].reshape(8, 16, 128).astype(BF)
            send2(i - 1)

        loop(16, twist)
        send2(15)

    loop(4, stage1)

    for j in range(8):
        x2[j, me] = y2[0, j]

    def send2b(k):
        p = peer(me, k)
        remote(y2.at[k, pl.ds(4, 4)], x2.at[pl.ds(4, 4), me], 4, 4, p).start()

    loop(N, send2b, 1)

    @pl.when(me > 0)
    def _():
        send_d(0, 1)

    for c in range(8):
        fw[c, me] = yd[me, c]

    @pl.when(me > 0)
    def _():
        for c in range(8):
            fw[c, H - me] = ym[me, c]

    @pl.when(me == 0)
    def _():
        wait_recv(2, nyq)

    for h in range(2):
        wait_recv(3 + h, x2.at[pl.ds(4 * h, 4), pl.ds(0, H)])

        @pl.when(me == 0)
        def _():
            wait_recv(1 + 10 * h, fw.at[pl.ds(4 * h, 4), pl.ds(0, N - 1)])

        @pl.when(me > 0)
        def _():
            wait_recv(1 + 10 * h, fw.at[pl.ds(4 * h, 4), pl.ds(0, N - 2)])

        cols = [x2[4 * h + j].reshape(1024, 128) for j in range(4)]
        for j in range(4):
            xb[:, j * 128 : (j + 1) * 128] = cols[j]

        def inner(first, ref, at):
            tab = t2[...].reshape(1024, 1024)
            if h == 0:
                part[:, at : at + 128] = dot(first[...].reshape(1024, 1024), ref[:, 0:128])
                part[:, at + 128 : at + 256] = dot(tab, ref[:, 128:256])
            else:
                part[:, at : at + 256] = dot(tab, ref[:, 0:256])
            part[:, at + 256 : at + 512] = dot(tab, ref[:, 256:512])

        inner(t2s, xb, 0)

        def stage2(g):
            def multiply(i):
                v = peer(me, g * 16 + i)
                r0 = pl.multiple_of(g * 256 + i * 16, 16)
                for j in range(4):
                    sr = part[pl.ds(r0, 8), j * 128 : (j + 1) * 128]
                    si = part[pl.ds(r0 + 8, 8), j * 128 : (j + 1) * 128]
                    f = fw[4 * h + j, v].astype(F32)
                    fre = f[0:8]
                    fim = f[8:16]
                    pr = sr * fre - si * fim
                    pi = -(sr * fim + si * fre)
                    prod[pl.ds(pl.multiple_of(v * 16, 16), 16), j * 128 : (j + 1) * 128] = (
                        jnp.concatenate([pr, pi], axis=0).astype(BF)
                    )

            loop(16, multiply)
            if h == 0:

                @pl.when((me == 0) & (g == 0))
                def _():
                    sr = part[0:8, 0:128]
                    si = part[8:16, 0:128]
                    f = fw[0, 0].astype(F32)
                    fre = f[0:8]
                    fim = f[8:16]
                    rows = lax.broadcasted_iota(jnp.int32, (8, 128), 0)
                    pr = sr * fre - si * fim
                    pi = -(sr * fim + si * fre)
                    pr = jnp.where(rows == 0, sr * fre, pr)
                    pi = jnp.where(rows == 0, -(si * nyq[...].astype(F32)[0:8]), pi)
                    prod[0:16, 0:128] = jnp.concatenate([pr, pi], axis=0).astype(BF)

        loop(4, stage2)

        inner(t3s, prod, 512)

        def stage3(g):
            def send3(i):
                k = g * 16 + i
                p = peer(me, k)

                @pl.when((k > 0) & (i >= 0))
                def _():
                    remote(
                        y3.at[k, pl.ds(4 * h, 4)], x4.at[me, pl.ds(4 * h, 4)], 5 + h, 5 + h, p
                    ).start()

            def untwist(i):
                k = g * 16 + i
                t = peer(me, k)
                r0 = pl.multiple_of(k * 16, 16)
                for j in range(4):
                    re = part[pl.ds(r0, 8), 512 + j * 128 : 640 + j * 128]
                    im = part[pl.ds(r0 + 8, 8), 512 + j * 128 : 640 + j * 128]
                    wc = wb[t, 4 * h + j]
                    ws = wb[t, 8 + 4 * h + j]
                    y3[k, 4 * h + j] = jnp.concatenate(
                        [re * wc + im * ws, re * ws - im * wc], axis=0
                    ).astype(BF)
                send3(i - 1)

            loop(16, untwist)
            send3(15)

        loop(4, stage3)
        for j in range(4):
            x4[me, 4 * h + j] = y3[0, 4 * h + j]

    for h in range(2):
        wait_recv(5 + h, x4.at[pl.ds(0, H), pl.ds(4 * h, 4)])

        def relay4(i):
            v = x4[pl.ds(i * 2, 2), 4 * h : 4 * h + 4].astype(F32).reshape(128, 128)
            tr[0:128, :] = v
            for b in range(8):
                xb[pl.ds(pl.multiple_of(h * 512 + i * 16, 16), 16), b * 128 : (b + 1) * 128] = tr[
                    pl.ds(b, 16, stride=8), :
                ].astype(BF)

        loop(32, relay4)

        def stage4(g):
            rows = pl.ds(pl.multiple_of(g * 256, 256), 256)
            acc[...] = part[rows, :] + dot(
                t4[pl.ds(g * 16, 16), :, 512:1024].reshape(256, 512), xb[512:1024, :]
            )

            def send4(i):
                k = g * 16 + i
                p = peer(me, k)

                @pl.when((k > 0) & (i >= 0))
                def _():
                    remote(y4.at[k], out_h.at[:, me], 7, 7, p).start()

            def finish(i):
                k = g * 16 + i
                r0 = pl.multiple_of(i * 16, 16)
                for b in range(8):
                    tr[pl.ds(b, 16, stride=8), :] = acc[pl.ds(r0, 16), b * 128 : (b + 1) * 128]
                y4[k] = (tr[0:128, :] * SCALE).reshape(16, 8, 128).astype(BF)
                send4(i - 1)

            loop(16, finish)
            send4(15)

        if h == 0:
            for j in range(4):
                cols = slice(j * 256, (j + 1) * 256)
                part[:, cols] = dot(t4[:, :, 0:512].reshape(1024, 512), xb[0:512, cols])
        else:
            loop(4, stage4)

    own4 = copy(y4.at[0], out_h.at[:, me], 10)
    own4.start()
    wait_send(0, sig_h.at[:, pl.ds(0, H)])
    near0 = near(me, 0)

    def drained(n):
        for h in range(2):
            wait_send(1 + h, yd.at[pl.ds(0, n), pl.ds(4 * h, 4)])

    @pl.when(me == 0)
    def _():
        drained(62)

    @pl.when((me > 0) & near0)
    def _():
        drained(61)

    @pl.when((me > 0) & jnp.logical_not(near0))
    def _():
        drained(63)

    @pl.when(me == 32)
    def _():
        wait_send(8, yq)

    for h in range(2):
        wait_send(3 + h, y2.at[pl.ds(0, H), pl.ds(4 * h, 4)])
        wait_send(5 + h, y3.at[pl.ds(0, H), pl.ds(4 * h, 4)])
    wait_send(7, y4.at[pl.ds(0, H)])
    wait_recv(7, out_h.at[:, pl.ds(0, H)])
    own4.wait()


def local(signal, gate_values, skip_gain, filter_spectrum):
    blocks, inner = make_tables()
    any_ = pl.BlockSpec(memory_space=pl.ANY)
    hbm = pl.BlockSpec(memory_space=pltpu.HBM)
    V = pltpu.VMEM
    dma = pltpu.SemaphoreType.DMA
    out = pl.pallas_call(
        kernel,
        out_shape=jax.ShapeDtypeStruct((16, 64, 8, 128), BF),
        in_specs=[hbm, hbm, hbm, hbm],
        out_specs=any_,
        scratch_shapes=[
            V((64, 16, 8, 128), BF),
            V((2, 8, 128, 8, 128), BF),
            V((64, 8, 16, 128), BF),
            V((64, 8, 16, 128), BF),
            V((16, 128), BF),
            V((8, 64, 16, 128), BF),
            V((64, 8, 16, 128), BF),
            V((64, 8, 16, 128), BF),
            V((64, 8, 16, 128), BF),
            V((64, 16, 8, 128), BF),
            V((64, 16, 1024), BF),
            V((64, 16, 1024), BF),
            V((64, 16, 1024), BF),
            V((64, 16, 1024), BF),
            V((64, 16, 1024), BF),
            V((64, 16, 8, 128), F32),
            V((8, 64, 16, 128), BF),
            V((16, 128), BF),
            V((1024, 1024), BF),
            V((1152, 128), F32),
            V((256, 1024), F32),
            V((1024, 512), BF),
            V((1024, 1024), F32),
            V((5, 2, N, 128), F32),
            V((6, 2, 16, 1024), F32),
            dma((9,)),
            dma((12,)),
            dma((12,)),
        ],
        compiler_params=pltpu.CompilerParams(
            collective_id=0, has_side_effects=True, vmem_limit_bytes=58 << 20
        ),
    )(
        signal.reshape(16, 64, 8, 128),
        filter_spectrum.reshape(2, 8, 128, 8, 128),
        jnp.asarray(blocks),
        jnp.asarray(inner),
    )
    grid = (16, 64, 8, 128)
    skipped = skip_gain * signal.reshape(grid).astype(F32)
    result = gate_values.reshape(grid).astype(F32) * (out.astype(F32) + skipped)
    return result.astype(BF).reshape(8192, 128)


def solution(mesh):
    return jax.shard_map(
        local,
        mesh=mesh,
        in_specs=(P("seq", "chan"), P("seq", "chan"), P("chan"), P(None, "seq", None, "chan")),
        out_specs=P("seq", "chan"),
        check_vma=False,
    )
```
